32 devices in a mesh: groups: 2 (over x), seq: 8 (over z, y), head: 2 (over core).
Axes of the slice: x: 2, y: 2, z: 4, core: 2. Of those that a mesh axis runs over, the one named last changes fastest.
Arguments:
- queries: bfloat16 [2048, 6144], P(('groups', 'seq', 'head')), parts along dimension 0, may hold values from -600 to 600
- latents: bfloat16 [2048, 576], P(('groups', 'seq')), parts along dimension 0, may hold values from -600 to 600
- latent_gain: float32 [512], replicated, may hold values from 0.1 to 1.9
- key_up: bfloat16 [32, 128, 512], P('head'), may hold values from -0.5 to 0.5
- value_up: bfloat16 [32, 512, 128], P('head'), may hold values from -1 to 1
- out_weight: bfloat16 [4096, 7168], P('head', 'seq'), may hold values from -0.09375 to 0.09375
Outputs:
- mixed: bfloat16 [16, 2, 64, 7168], P('groups', 'head', None, 'seq'), parts along dimension 0
The draws below stay inside these ranges and needn't reach their ends.
There are 2 independent parts, one for each index of `groups`. The reference program is written for one: setup_inputs(seed, part) draws one part's arguments, and reference() takes and returns one part's arrays. A program takes and returns all parts, laid end to end along the dimension named above; an argument that names none is the same for every part. Nothing has to cross between parts.
All inputs are finite; a program needn't handle non-finite values.
Results may differ from the reference program's by a relative error of at most 0.013.
Values may be sent and summed in bfloat16 or wider, within the bound.
No kernel may reach another device: no remote copies, remote signals or barrier semaphores. Data moves between devices by JAX's collectives and lax.ppermute only.
A program may use at most 128 MiB of HBM per device.

```python
import jax
import jax.numpy as jnp
from jax import lax

D = 7168
KV = 512
NOPE = 128
VD = 128
QK = 192
LATENT = 576
HEADS = 32
TOKENS = 1024
BLOCKS = 8
HSPLIT = 2
TOK_PIECE = 64


def draw_both(key):
    base_key = jax.random.fold_in(key, 7)
    keys = jax.random.split(base_key, 2)
    latent_vals = jnp.clip(jax.random.normal(keys[0], (TOKENS, LATENT), jnp.float32), -6.0, 6.0)
    query_vals = jnp.clip(jax.random.normal(keys[1], (TOKENS, HEADS * QK), jnp.float32), -6.0, 6.0)
    return (latent_vals, query_vals)


def draw_queries(key, part):
    return draw_both(key)[1].astype(jnp.bfloat16)


def draw_latents(key, part):
    return draw_both(key)[0].astype(jnp.bfloat16)


def block_levels(stream_key, shape, cuts, low, largest):
    gain = 1.0
    for dim, shards_of in cuts:
        draws = jax.random.uniform(jax.random.fold_in(jax.random.fold_in(stream_key, 6), dim), (shards_of,), jnp.float32, low / len(cuts), largest / len(cuts))
        gain = gain * jnp.repeat(jnp.exp(draws), shape[dim] // shards_of).reshape((-1,) + (1,) * (len(shape) - 1 - dim))
    return gain


def gaussian(rng, extent, deviation, limit, pieces=(), held_as=jnp.bfloat16):
    entries = deviation * jax.random.normal(rng, extent, jnp.float32)
    if pieces:
        entries = entries * block_levels(rng, extent, pieces, -0.22, 0.18)
    return jnp.clip(entries, -limit, limit).astype(held_as)


def setup_inputs(seed: int = 0, part: int = 0) -> dict:
    splits = jax.random.split(jax.random.key(seed), 7)
    part_splits = jax.random.split(jax.random.fold_in(splits[6], part), 7)
    queries = draw_queries(jax.random.fold_in(jax.random.fold_in(splits[6], part), 71), part)
    latents = draw_latents(jax.random.fold_in(jax.random.fold_in(splits[6], part), 71), part)
    latent_gain = jnp.clip(1.0 + 0.18 * jax.random.normal(splits[2], (KV,), jnp.float32), 0.1, 1.9)
    key_up = gaussian(splits[3], (HEADS, NOPE, KV), NOPE ** -0.5, 0.5, ((0, 2),))
    value_up = gaussian(splits[4], (HEADS, KV, VD), (KV // 16) ** -0.5, 1.0, ((0, 2),))
    out_weight = gaussian(splits[5], (HEADS * VD, D), (HEADS * VD) ** -0.5, 0.09375, ((0, 2), (1, 8)))
    return {"queries": queries, "latents": latents, "latent_gain": latent_gain, "key_up": key_up, "value_up": value_up, "out_weight": out_weight}


def rotate(values, position):
    middle = values.shape[-1] // 2
    frequency = 10000.0 ** (-jnp.arange(middle, dtype=jnp.float32) / middle)
    angles = position[..., None] * frequency
    former = values[..., :middle]
    latter = values[..., middle:]
    cosine = jnp.cos(angles)
    sin_part = jnp.sin(angles)
    return jnp.concatenate([former * cosine - latter * sin_part, former * sin_part + latter * cosine], -1)

def reference(queries, latents, latent_gain, key_up, value_up, out_weight):
    positions = jnp.arange(TOKENS).astype(jnp.float32)
    latent_f = latents.astype(jnp.float32)
    compressed = latent_f[:, :KV]
    spread = lax.optimization_barrier(jnp.mean(compressed * compressed, axis=-1, keepdims=True))
    normed = compressed * lax.rsqrt(spread + 1e-06) * latent_gain
    key_rope = rotate(latent_f[:, KV:], positions)
    key_rows = jnp.concatenate([normed, key_rope], -1).astype(jnp.bfloat16)
    query = queries.reshape(TOKENS, HEADS, QK)
    latent_query = jnp.einsum('thd,hdc->thc', query[..., :NOPE].astype(jnp.float32), key_up.astype(jnp.float32)).astype(jnp.bfloat16)
    rope_query = rotate(query[..., NOPE:].astype(jnp.float32), positions[:, None]).astype(jnp.bfloat16)
    query_rows = jnp.concatenate([latent_query, rope_query], -1)
    scale = QK ** (-0.5)
    visible = jnp.arange(TOKENS)[None, :] <= jnp.arange(TOKENS)[:, None]
    values = key_rows[:, :KV]

    def one_head(pair):
        head_query, head_value = pair
        scores = jnp.dot(head_query, key_rows.T, preferred_element_type=jnp.float32) * scale
        peak = lax.optimization_barrier(jnp.max(jnp.where(visible, scores, -1e+30), axis=-1))
        probs = jnp.where(visible, jnp.exp(scores - peak[:, None]), 0.0).astype(jnp.bfloat16)
        totals = lax.optimization_barrier(jnp.sum(probs.astype(jnp.float32), axis=-1))
        latent_out = (jnp.dot(probs, values, preferred_element_type=jnp.float32) / totals[:, None]).astype(jnp.bfloat16)
        return jnp.dot(latent_out, head_value, preferred_element_type=jnp.float32).astype(jnp.bfloat16)
    heads = lax.map(one_head, (jnp.transpose(query_rows, (1, 0, 2)), value_up))
    heads_out = jnp.transpose(heads, (1, 0, 2)).reshape(TOKENS, HEADS * VD)
    mixed = jnp.dot(heads_out, out_weight, preferred_element_type=jnp.float32).astype(jnp.bfloat16)
    return mixed.reshape(BLOCKS, HSPLIT, TOK_PIECE, D)
```

```python
import functools

import jax
import jax.numpy as jnp
import numpy as np
from jax import lax
from jax.experimental import pallas as pl
from jax.experimental.pallas import tpu as pltpu
from jax.sharding import PartitionSpec as P

KV = 512
ROPE = 64
NOPE = 128
VD = 128
QK = NOPE + ROPE
WIDE = KV + 2 * ROPE
EPS = 1e-06


def rope_table(total):
    middle = ROPE // 2
    frequency = (10000.0 ** (-np.arange(middle, dtype=np.float32) / middle)).astype(np.float32)
    angles = (np.arange(total, dtype=np.float32)[:, None] * frequency).astype(np.float64)
    cosine, sine = np.cos(angles), np.sin(angles)
    return np.concatenate([cosine, cosine, -sine, sine], -1).astype(np.float32)


def rotate(values, table):
    middle = ROPE // 2
    swapped = jnp.concatenate([values[:, middle:], values[:, :middle]], -1)
    return values * table[:, :ROPE] + swapped * table[:, ROPE:]


def prepare_kernel(half, where, latents, gain, table, full_out, half_out):
    latent_f = latents[...].astype(jnp.float32)
    compressed = latent_f[:, :KV]
    spread = jnp.mean(compressed * compressed, axis=-1, keepdims=True)
    normed = compressed * lax.rsqrt(spread + EPS) * gain[...]
    full_out[:, :KV] = normed.astype(jnp.bfloat16)
    rope = rotate(latent_f[:, KV:], table[...]).astype(jnp.bfloat16)
    full_out[:, KV:] = jnp.concatenate([rope, jnp.zeros_like(rope)], -1)
    half_out[...] = full_out[pl.ds(pl.multiple_of(where[0] * half, half), half), :]


def prepare(where, latents, gain, table):
    rows = latents.shape[0]
    half = rows // 2
    return pl.pallas_call(
        functools.partial(prepare_kernel, half),
        grid_spec=pltpu.PrefetchScalarGridSpec(
            num_scalar_prefetch=1,
            grid=(1,),
            in_specs=[
                pl.BlockSpec((rows, KV + ROPE), lambda i, w: (0, 0)),
                pl.BlockSpec((1, KV), lambda i, w: (0, 0)),
                pl.BlockSpec((rows, 2 * ROPE), lambda i, w: (w[1], 0)),
            ],
            out_specs=[
                pl.BlockSpec((rows, WIDE), lambda i, w: (0, 0)),
                pl.BlockSpec((half, WIDE), lambda i, w: (0, 0)),
            ],
        ),
        out_shape=[
            jax.ShapeDtypeStruct((rows, WIDE), jnp.bfloat16),
            jax.ShapeDtypeStruct((half, WIDE), jnp.bfloat16),
        ],
        name="prepare",
    )(where, latents, gain, table)


def lift_kernel(heads, where, queries, key_up, table, out):
    rows = queries.shape[0]
    for head in range(heads):
        start = head * QK
        plain = queries[:, start : start + NOPE]
        lifted = jnp.dot(plain, key_up[head], preferred_element_type=jnp.float32)
        turned = rotate(queries[:, start + NOPE : start + QK].astype(jnp.float32), table[...])
        turned = turned.astype(jnp.bfloat16)
        out[pl.ds(head * rows, rows), :KV] = lifted.astype(jnp.bfloat16)
        out[pl.ds(head * rows, rows), KV:] = jnp.concatenate([turned, jnp.zeros_like(turned)], -1)


def lift(where, queries, key_up, table, other):
    rows = queries.shape[0]
    heads = key_up.shape[0]
    step = 4
    steps = heads // step

    def query_block(i, w):
        return (0, (1 - w[0] if other else w[0]) * steps + i)

    return pl.pallas_call(
        functools.partial(lift_kernel, step),
        grid_spec=pltpu.PrefetchScalarGridSpec(
            num_scalar_prefetch=1,
            grid=(steps,),
            in_specs=[
                pl.BlockSpec((rows, step * QK), query_block),
                pl.BlockSpec((step, NOPE, KV), lambda i, w: (i, 0, 0)),
                pl.BlockSpec((rows, 2 * ROPE), lambda i, w: (2 * w[1] + w[0], 0)),
            ],
            out_specs=pl.BlockSpec((step * rows, WIDE), lambda i, w: (i, 0)),
        ),
        out_shape=jax.ShapeDtypeStruct((heads * rows, WIDE), jnp.bfloat16),
        cost_estimate=pl.CostEstimate(
            flops=2 * heads * rows * NOPE * KV,
            bytes_accessed=2 * heads * (NOPE * KV + rows * (QK + WIDE)),
            transcendentals=0,
        ),
        name="lift",
    )(where, queries, key_up, table)


def attend_kernel(heads, groups, where, query_rows, value_up, key_pos, *rest):
    keys, out = rest[:groups], rest[groups]
    total = query_rows.shape[0]
    rows = total // heads
    query = query_rows[...]
    first = where[1] * 2 * rows + where[0] * rows
    query_pos = first + lax.rem(lax.broadcasted_iota(jnp.int32, (total, 1), 0), rows)
    scores = []
    start = 0
    peak = None
    for group in keys:
        width = group.shape[0]
        score = lax.dot_general(
            query, group[...], (((1,), (1,)), ((), ())), preferred_element_type=jnp.float32
        )
        visible = key_pos[:, start : start + width] <= query_pos
        score = jnp.where(visible, score, -1e30)
        best = jnp.max(score, axis=-1, keepdims=True)
        peak = best if peak is None else jnp.maximum(peak, best)
        scores.append(score)
        start += width
    factor = QK ** (-0.5)
    sums = jnp.zeros((total, KV), jnp.float32)
    totals = jnp.zeros((total, 1), jnp.float32)
    for group, score in zip(keys, scores):
        probs = jnp.exp((score - peak) * factor).astype(jnp.bfloat16)
        totals += jnp.sum(probs.astype(jnp.float32), axis=-1, keepdims=True)
        sums += jnp.dot(probs, group[:, :KV], preferred_element_type=jnp.float32)
    latent_out = (sums / totals).astype(jnp.bfloat16)
    for head in range(heads):
        piece = jnp.dot(
            latent_out[head * rows : (head + 1) * rows],
            value_up[head],
            preferred_element_type=jnp.float32,
        )
        out[:, head * VD : (head + 1) * VD] = piece.astype(jnp.bfloat16)


def attend(where, query_rows, value_up, key_pos, keys, rows):
    heads = value_up.shape[0]
    step = 4
    steps = heads // step
    key_total = key_pos.shape[1]
    return pl.pallas_call(
        functools.partial(attend_kernel, step, len(keys)),
        grid_spec=pltpu.PrefetchScalarGridSpec(
            num_scalar_prefetch=1,
            grid=(steps,),
            in_specs=[
                pl.BlockSpec((step * rows, WIDE), lambda i, w: (i, 0)),
                pl.BlockSpec((step, KV, VD), lambda i, w: (i, 0, 0)),
                pl.BlockSpec((1, key_total), lambda i, w: (0, 0)),
            ]
            + [pl.BlockSpec(key.shape, lambda i, w: (0, 0)) for key in keys],
            out_specs=pl.BlockSpec((rows, step * VD), lambda i, w: (0, i)),
        ),
        out_shape=jax.ShapeDtypeStruct((rows, heads * VD), jnp.bfloat16),
        cost_estimate=pl.CostEstimate(
            flops=2 * heads * rows * (key_total * (WIDE + KV) + KV * VD),
            bytes_accessed=2 * heads * (KV * VD + rows * (WIDE + VD)) + 2 * key_total * WIDE,
            transcendentals=heads * rows * key_total,
        ),
        name="attend",
    )(where, query_rows, value_up, key_pos, *keys)


def gather_plan(count):
    moves = []
    bit = count // 2
    slots = [0]
    while bit:
        moves += [(slot, bit) for slot in slots]
        slots += [slot | bit for slot in slots]
        bit //= 2
    needed = {(d, m) for d in range(count) for m in range(1, count) if d ^ m < d}
    plan = []
    for slot, bit in reversed(moves):
        receivers = [d for d in range(count) if (d, slot | bit) in needed]
        if slot:
            needed |= {(d ^ bit, slot) for d in receivers}
        plan.append((slot, bit, receivers))
    return plan[::-1]


def local(queries, latents, latent_gain, key_up, value_up, out_weight):
    seq_count = lax.axis_size("seq")
    head_count = lax.axis_size("head")
    seq_index = lax.axis_index("seq")
    head_index = lax.axis_index("head")
    rows = queries.shape[0]
    tok_block = latents.shape[0]
    where = jnp.where(jnp.arange(2) == 0, head_index, seq_index).astype(jnp.int32)
    table = jnp.asarray(rope_table(seq_count * tok_block))
    swap_pairs = [(i, (i + 1) % head_count) for i in range(head_count)]

    def swap(value):
        return lax.ppermute(value, "head", swap_pairs)

    own_keys, half_keys = prepare(where, latents, latent_gain.reshape(1, KV), table)
    slots = {0: half_keys}
    for slot, bit, receivers in gather_plan(seq_count):
        slots[slot | bit] = lax.ppermute(slots[slot], "seq", [(d ^ bit, d) for d in receivers])
    near = [m for m in range(1, seq_count) if m % 2 == 0] + [1]
    far = [m for m in range(2, seq_count) if m % 2 == 1]
    near_keys = jnp.concatenate([slots[m] for m in near], 0)
    far_keys = jnp.concatenate([slots[m] for m in far], 0)
    keys = [own_keys, near_keys, far_keys, swap(near_keys), swap(far_keys)]
    block_of = np.concatenate(
        [np.repeat(np.array(part, np.int32), rows) for part in ([0, 0], near, far, near, far)]
    )
    side_of = np.concatenate(
        [
            np.repeat(np.array(part, np.int32), rows)
            for part in ([0, 0], [0] * len(near + far), [1] * len(near + far))
        ]
    )
    fixed = np.zeros(block_of.shape, np.int32)
    fixed[rows : 2 * rows] = rows
    inner = np.arange(block_of.size, dtype=np.int32) % rows
    moved = np.arange(block_of.size) >= 2 * rows
    key_pos = (
        (seq_index ^ block_of) * tok_block
        + jnp.where(moved, (head_index ^ side_of) * rows, fixed)
        + inner
    ).astype(jnp.int32)[None, :]

    key_other, value_other, weight_other = swap(key_up), swap(value_up), swap(out_weight)
    rows_a = lift(where, queries, key_up, table, False)
    heads_a = attend(where, rows_a, value_up, key_pos, keys, rows)
    rows_b = lift(where, queries, key_other, table, True)
    heads_b = attend(where, rows_b, value_other, key_pos, keys, rows)

    order = list(range(0, seq_count, 2)) + list(range(seq_count - 1, 0, -2))
    place = {device: i for i, device in enumerate(order)}
    right = [(order[i], order[(i + 1) % seq_count]) for i in range(seq_count)]
    left = [(b, a) for a, b in right]
    steps = seq_count // 2
    source = np.array(
        [[order[(place[d] + k) % seq_count] for k in range(seq_count)] for d in range(seq_count)],
        np.int32,
    )
    sources = jnp.asarray(source)[seq_index]

    def project(first, second):
        return (
            jnp.dot(first, out_weight, preferred_element_type=jnp.float32)
            + jnp.dot(second, weight_other, preferred_element_type=jnp.float32)
        ).astype(jnp.bfloat16)

    mixed = jnp.zeros((seq_count, 1, rows, out_weight.shape[1]), jnp.bfloat16)

    def put(mixed, piece, offset):
        return lax.dynamic_update_slice(
            mixed, piece[None, None], (sources[offset % seq_count], 0, 0, 0)
        )

    mixed = put(mixed, project(heads_a, heads_b), 0)
    right_a, right_b, left_a, left_b = heads_a, heads_b, heads_a, heads_b
    for step in range(1, steps + 1):
        last = step == steps
        right_a = lax.ppermute(right_a, "seq", right)
        if not last:
            left_a = lax.ppermute(left_a, "seq", left)
            right_b = lax.ppermute(right_b, "seq", right)
        left_b = lax.ppermute(left_b, "seq", left)
        if last:
            mixed = put(mixed, project(right_a, left_b), step)
        else:
            mixed = put(mixed, project(right_a, right_b), -step)
            mixed = put(mixed, project(left_a, left_b), step)
    return mixed


def solution(mesh):
    placed = (
        P(("groups", "seq", "head"), None),
        P(("groups", "seq"), None),
        P(),
        P("head", None, None),
        P("head", None, None),
        P("head", "seq"),
    )
    return jax.shard_map(
        local,
        mesh=mesh,
        in_specs=placed,
        out_specs=P("groups", "head", None, "seq"),
        check_vma=False,
    )
```

```python
import functools

import jax
import jax.numpy as jnp
import numpy as np
from jax import lax
from jax.experimental import pallas as pl
from jax.experimental.pallas import tpu as pltpu
from jax.sharding import PartitionSpec as P


KV = 512
ROPE = 64
NOPE = 128
VD = 128
QK = NOPE + ROPE
WIDE = KV + 2 * ROPE
EPS = 1e-06
HIDDEN = -1e30


def rope_table(total):
    middle = ROPE // 2
    frequency = (10000.0 ** (-np.arange(middle, dtype=np.float32) / middle)).astype(np.float32)
    angles = (np.arange(total, dtype=np.float32)[:, None] * frequency).astype(np.float64)
    cosine, sine = np.cos(angles), np.sin(angles)
    return np.concatenate([cosine, cosine, -sine, sine], -1).astype(np.float32)


def rotate(values, table):
    middle = ROPE // 2
    swapped = jnp.concatenate([values[:, middle:], values[:, :middle]], -1)
    return values * table[:, :ROPE] + swapped * table[:, ROPE:]


def tag_lanes(rows, value):
    lane = lax.broadcasted_iota(jnp.int32, (rows, ROPE), 1)
    return value(lane).astype(jnp.bfloat16)


def prepare_kernel(half, latents, gain, table, full_out, half_out):
    block = lax.axis_index("seq")
    latent_f = latents[...].astype(jnp.float32)
    tokens = latent_f.shape[1]
    compressed = latent_f[:KV]
    spread = jnp.mean(compressed * compressed, axis=0, keepdims=True)
    normed = (compressed * lax.rsqrt(spread + EPS)).T * gain[...]
    full_out[:, :KV] = normed.astype(jnp.bfloat16)
    here = table[pl.ds(pl.multiple_of(block * tokens, tokens), tokens), :]
    rope = rotate(latent_f[KV:].T, here).astype(jnp.bfloat16)
    tags = tag_lanes(tokens, lambda lane: jnp.where(lane == block, 1.0, 0.0))
    full_out[:, KV:] = jnp.concatenate([rope, tags], -1)
    start = lax.axis_index("head") * half
    half_out[...] = full_out[pl.ds(pl.multiple_of(start, half), half), :]


def prepare(latents, gain, table):
    rows = latents.shape[1]
    half = rows // 2
    return pl.pallas_call(
        functools.partial(prepare_kernel, half),
        out_shape=[
            jax.ShapeDtypeStruct((rows, WIDE), jnp.bfloat16),
            jax.ShapeDtypeStruct((half, WIDE), jnp.bfloat16),
        ],
        cost_estimate=pl.CostEstimate(
            flops=10**8, bytes_accessed=4 * rows * WIDE, transcendentals=rows
        ),
        compiler_params=pltpu.CompilerParams(vmem_limit_bytes=12 << 20),
        name="prepare",
    )(latents, gain, table)


def lift_kernel(queries, key_up, table, out):
    rows = queries.shape[0]
    heads = key_up.shape[0]
    block = lax.axis_index("seq")
    first = pl.multiple_of((2 * block + lax.axis_index("head")) * rows, rows)
    for head in range(heads):
        plain = queries[:, head * QK : head * QK + NOPE]
        lifted = jnp.dot(plain, key_up[head], preferred_element_type=jnp.float32)
        out[pl.ds(head * rows, rows), :KV] = lifted.astype(jnp.bfloat16)
    turning = jnp.concatenate(
        [
            queries[:, head * QK + NOPE : (head + 1) * QK].astype(jnp.float32)
            for head in range(heads)
        ],
        0,
    )
    here = jnp.concatenate([table[pl.ds(first, rows), :]] * heads, 0)
    turned = rotate(turning, here).astype(jnp.bfloat16)
    tags = tag_lanes(heads * rows, lambda lane: jnp.where(lane > block, HIDDEN, 0.0))
    out[:, KV:] = jnp.concatenate([turned, tags], -1)


def lift(queries, key_up, table, other):
    rows = queries.shape[0]
    heads = key_up.shape[0]
    step = 8
    steps = heads // step

    def query_block(i):
        half = lax.axis_index("head")
        return (0, (1 - half if other else half) * steps + i)

    return pl.pallas_call(
        lift_kernel,
        grid=(steps,),
        in_specs=[
            pl.BlockSpec((rows, step * QK), query_block),
            pl.BlockSpec((step, NOPE, KV), lambda i: (i, 0, 0)),
            pl.BlockSpec(table.shape, lambda i: (0, 0)),
        ],
        out_specs=pl.BlockSpec((step * rows, WIDE), lambda i: (i, 0)),
        out_shape=jax.ShapeDtypeStruct((heads * rows, WIDE), jnp.bfloat16),
        cost_estimate=pl.CostEstimate(
            flops=2 * heads * rows * NOPE * KV,
            bytes_accessed=2 * heads * (NOPE * KV + rows * (QK + WIDE)),
            transcendentals=0,
        ),
        compiler_params=pltpu.CompilerParams(vmem_limit_bytes=12 << 20),
        name="lift",
    )(queries, key_up, table)


def attend_kernel(part, groups, query_rows, value_up, *rest):
    groups, (out, keys) = rest[:groups], rest[groups:]
    total = query_rows.shape[0]
    heads = value_up.shape[0]
    rows = total // heads
    own = groups[0].shape[0]

    @pl.when(pl.program_id(0) == 0)
    def _():
        start = 0
        for group in groups:
            keys[start : start + group.shape[0], :] = group[...]
            start += group.shape[0]

    factor = QK ** (-0.5) * float(np.log2(np.e))
    offset = lax.axis_index("head") * rows

    def score_rows(i):
        return lax.dot_general(
            query_rows[i * part : (i + 1) * part, :],
            keys[...],
            (((1,), (1,)), ((), ())),
            preferred_element_type=jnp.float32,
        )

    def finish(i, score):
        query_pos = offset + lax.rem(lax.broadcasted_iota(jnp.int32, (part, own), 0), rows)
        key_pos = lax.broadcasted_iota(jnp.int32, (part, own), 1)
        diagonal = jnp.where(key_pos <= query_pos, score[:, :own], HIDDEN)
        score = jnp.concatenate([diagonal, score[:, own:]], 1)
        peak = jnp.max(score, axis=-1, keepdims=True)
        probs = jnp.exp2((score - peak) * factor)
        totals = jnp.sum(probs, axis=-1, keepdims=True)
        sums = jnp.dot(
            probs.astype(jnp.bfloat16), keys[:, :KV], preferred_element_type=jnp.float32
        )
        latent_out = (sums / totals).astype(jnp.bfloat16)
        for j in range(part // rows):
            head = i * (part // rows) + j
            piece = jnp.dot(
                latent_out[j * rows : (j + 1) * rows],
                value_up[head],
                preferred_element_type=jnp.float32,
            )
            out[:, head * VD : (head + 1) * VD] = piece.astype(jnp.bfloat16)

    count = total // part
    score = score_rows(0)
    for i in range(count):
        later = score_rows(i + 1) if i + 1 < count else None
        finish(i, score)
        score = later


def attend(query_rows, value_up, keys, rows):
    heads = value_up.shape[0]
    step = 8
    steps = heads // step
    key_total = sum(key.shape[0] for key in keys)
    return pl.pallas_call(
        functools.partial(attend_kernel, 4 * rows, len(keys)),
        grid=(steps,),
        in_specs=[
            pl.BlockSpec((step * rows, WIDE), lambda i: (i, 0)),
            pl.BlockSpec((step, KV, VD), lambda i: (i, 0, 0)),
        ]
        + [pl.BlockSpec(key.shape, lambda i: (0, 0)) for key in keys],
        out_specs=pl.BlockSpec((rows, step * VD), lambda i: (0, i)),
        out_shape=jax.ShapeDtypeStruct((rows, heads * VD), jnp.bfloat16),
        scratch_shapes=[pltpu.VMEM((key_total, WIDE), jnp.bfloat16)],
        cost_estimate=pl.CostEstimate(
            flops=2 * heads * rows * (key_total * (WIDE + KV) + KV * VD),
            bytes_accessed=2 * heads * (KV * VD + rows * (WIDE + VD)) + 2 * key_total * WIDE,
            transcendentals=heads * rows * key_total,
        ),
        compiler_params=pltpu.CompilerParams(
            vmem_limit_bytes=(12 << 20) + 16 * key_total * WIDE
        ),
        name="attend",
    )(query_rows, value_up, *keys)


def gather_plan(count):
    moves = []
    bit = count // 2
    slots = [0]
    while bit:
        moves += [(slot, bit) for slot in slots]
        slots += [slot | bit for slot in slots]
        bit //= 2
    return moves


def layer(queries, latents, latent_gain, key_up, value_up, out_weight):
    seq_count = lax.axis_size("seq")
    head_count = lax.axis_size("head")
    seq_index = lax.axis_index("seq")
    rows = queries.shape[0]
    tok_block = latents.shape[0]
    table = jnp.asarray(rope_table(seq_count * tok_block))
    swap_pairs = [(i, (i + 1) % head_count) for i in range(head_count)]
    everyone = range(seq_count)

    own_keys, half_keys = prepare(latents.T, latent_gain.reshape(1, KV), table)
    slots = {0: half_keys}
    for slot, bit in gather_plan(seq_count):
        slots[slot | bit] = lax.ppermute(slots[slot], "seq", [(d ^ bit, d) for d in everyone])
    near = [m for m in range(1, seq_count) if m % 2 == 0] + [1]
    far = [m for m in range(2, seq_count) if m % 2 == 1]
    near_keys = jnp.concatenate([slots[m] for m in near], 0)
    far_keys = jnp.concatenate([slots[m] for m in far], 0)
    near_swap = lax.ppermute(near_keys, "head", swap_pairs)
    far_swap = lax.ppermute(far_keys, "head", swap_pairs)
    keys = [own_keys, near_keys, far_keys, near_swap, far_swap]

    key_other = lax.ppermute(key_up, "head", swap_pairs)
    value_other = lax.ppermute(value_up, "head", swap_pairs)
    weight_other = lax.ppermute(out_weight, "head", swap_pairs)
    rows_a = lift(queries, key_up, table, False)
    heads_a = attend(rows_a, value_up, keys, rows)
    rows_b = lift(queries, key_other, table, True)
    heads_b = attend(rows_b, value_other, keys, rows)

    order = list(range(0, seq_count, 2)) + list(range(seq_count - 1, 0, -2))
    place = {device: i for i, device in enumerate(order)}
    right = [(order[i], order[(i + 1) % seq_count]) for i in everyone]
    left = [(b, a) for a, b in right]
    steps = seq_count // 2
    source = np.array(
        [[order[(place[d] + k) % seq_count] for k in everyone] for d in everyone], np.int32
    )
    sources = jnp.asarray(source)[seq_index]

    def project(first, second):
        return (
            jnp.dot(first, out_weight, preferred_element_type=jnp.float32)
            + jnp.dot(second, weight_other, preferred_element_type=jnp.float32)
        ).astype(jnp.bfloat16)

    mixed = jnp.zeros((seq_count, 1, rows, out_weight.shape[1]), jnp.bfloat16)

    def put(mixed, first, second, offset):
        return lax.dynamic_update_slice(
            mixed,
            project(first, second)[None, None],
            (sources[offset % seq_count], 0, 0, 0),
        )

    right_a, right_b, left_a, left_b = heads_a, heads_b, heads_a, heads_b
    mixed = put(mixed, heads_a, heads_b, 0)
    for step in range(1, steps + 1):
        last = step == steps
        right_a = lax.ppermute(right_a, "seq", right)
        if not last:
            left_a = lax.ppermute(left_a, "seq", left)
            right_b = lax.ppermute(right_b, "seq", right)
        left_b = lax.ppermute(left_b, "seq", left)
        if last:
            mixed = put(mixed, right_a, left_b, step)
        else:
            mixed = put(mixed, right_a, right_b, -step)
            mixed = put(mixed, left_a, left_b, step)
    return mixed


def solution(mesh):
    placed = (
        P(("groups", "seq", "head"), None),
        P(("groups", "seq"), None),
        P(),
        P("head", None, None),
        P("head", None, None),
        P("head", "seq"),
    )
    return jax.shard_map(
        layer,
        mesh=mesh,
        in_specs=placed,
        out_specs=P("groups", "head", None, "seq"),
        check_vma=False,
    )
```

```python
import functools

import jax
import jax.numpy as jnp
import numpy as np
from jax import lax
from jax.experimental import pallas as pl
from jax.experimental.pallas import tpu as pltpu
from jax.sharding import PartitionSpec as P


KV = 512
ROPE = 64
NOPE = 128
VD = 128
QK = NOPE + ROPE
WIDE = KV + 2 * ROPE
EPS = 1e-06
HIDDEN = -1e30


def rope_angles(position, index):
    middle = ROPE // 2
    frequency = jnp.ones(index.shape, jnp.float32)
    for bit in range(middle.bit_length() - 1):
        factor = float(10000.0 ** (-(1 << bit) / middle))
        frequency *= jnp.where((index >> bit) % 2 == 1, factor, 1.0)
    return position.astype(jnp.float32) * frequency


def tag_lanes(rows, value):
    lane = lax.broadcasted_iota(jnp.int32, (rows, ROPE), 1)
    return value(lane).astype(jnp.bfloat16)


def prepare_kernel(half, latents, gain, full_out, half_out):
    block = lax.axis_index("seq")
    latent_f = latents[...].astype(jnp.float32)
    tokens = latent_f.shape[1]
    compressed = latent_f[:KV]
    spread = jnp.mean(compressed * compressed, axis=0, keepdims=True)
    normed = (compressed * lax.rsqrt(spread + EPS)).T * gain[...]
    full_out[:, :KV] = normed.astype(jnp.bfloat16)
    shape = (ROPE // 2, tokens)
    position = block * tokens + lax.broadcasted_iota(jnp.int32, shape, 1)
    angles = rope_angles(position, lax.broadcasted_iota(jnp.int32, shape, 0))
    cosine, sine = jnp.cos(angles), jnp.sin(angles)
    former, latter = latent_f[KV : KV + ROPE // 2], latent_f[KV + ROPE // 2 :]
    halves = [former * cosine - latter * sine, former * sine + latter * cosine]
    rope = jnp.concatenate(halves, 0).T.astype(jnp.bfloat16)
    tags = tag_lanes(tokens, lambda lane: jnp.where(lane == block, 1.0, 0.0))
    full_out[:, KV:] = jnp.concatenate([rope, tags], -1)
    start = lax.axis_index("head") * half
    half_out[...] = full_out[pl.ds(pl.multiple_of(start, half), half), :]


def prepare(latents, gain):
    rows = latents.shape[1]
    half = rows // 2
    return pl.pallas_call(
        functools.partial(prepare_kernel, half),
        out_shape=[
            jax.ShapeDtypeStruct((rows, WIDE), jnp.bfloat16),
            jax.ShapeDtypeStruct((half, WIDE), jnp.bfloat16),
        ],
        compiler_params=pltpu.CompilerParams(vmem_limit_bytes=12 << 20),
        cost_estimate=pl.CostEstimate(
            flops=10**8, bytes_accessed=4 * rows * WIDE, transcendentals=rows
        ),
        name="prepare",
    )(latents, gain)


def lift_kernel(queries, key_up, out):
    rows = queries.shape[0]
    heads = key_up.shape[0]
    block = lax.axis_index("seq")
    for head in range(heads):
        plain = queries[:, head * QK : head * QK + NOPE]
        lifted = jnp.dot(plain, key_up[head], preferred_element_type=jnp.float32)
        out[pl.ds(head * rows, rows), :KV] = lifted.astype(jnp.bfloat16)
    shape = (rows, ROPE)
    first = (2 * block + lax.axis_index("head")) * rows
    position = first + lax.broadcasted_iota(jnp.int32, shape, 0)
    lane = lax.broadcasted_iota(jnp.int32, shape, 1)
    upper = lane >= ROPE // 2
    angles = rope_angles(position, jnp.where(upper, lane - ROPE // 2, lane))
    cosine = jnp.concatenate([jnp.cos(angles)] * heads, 0)
    sine = jnp.sin(angles)
    sine = jnp.concatenate([jnp.where(upper, sine, -sine)] * heads, 0)
    turning = jnp.concatenate(
        [
            queries[:, head * QK + NOPE : (head + 1) * QK].astype(jnp.float32)
            for head in range(heads)
        ],
        0,
    )
    swapped = jnp.concatenate([turning[:, ROPE // 2 :], turning[:, : ROPE // 2]], -1)
    turned = (turning * cosine + swapped * sine).astype(jnp.bfloat16)
    tags = tag_lanes(heads * rows, lambda lane: jnp.where(lane > block, HIDDEN, 0.0))
    out[:, KV:] = jnp.concatenate([turned, tags], -1)


def lift(queries, key_up, other):
    rows = queries.shape[0]
    heads = key_up.shape[0]
    step = 8
    steps = heads // step

    def query_block(i):
        half = lax.axis_index("head")
        return (0, (1 - half if other else half) * steps + i)

    return pl.pallas_call(
        lift_kernel,
        grid=(steps,),
        in_specs=[
            pl.BlockSpec((rows, step * QK), query_block),
            pl.BlockSpec((step, NOPE, KV), lambda i: (i, 0, 0)),
        ],
        out_specs=pl.BlockSpec((step * rows, WIDE), lambda i: (i, 0)),
        out_shape=jax.ShapeDtypeStruct((heads * rows, WIDE), jnp.bfloat16),
        cost_estimate=pl.CostEstimate(
            flops=2 * heads * rows * NOPE * KV,
            bytes_accessed=2 * heads * (NOPE * KV + rows * (QK + WIDE)),
            transcendentals=0,
        ),
        compiler_params=pltpu.CompilerParams(vmem_limit_bytes=12 << 20),
        name="lift",
    )(queries, key_up)


def attend_kernel(part, groups, query_rows, value_up, *rest):
    groups, (out, keys) = rest[:groups], rest[groups:]
    total = query_rows.shape[0]
    heads = value_up.shape[0]
    rows = total // heads
    own = groups[0].shape[0]

    @pl.when(pl.program_id(0) == 0)
    def _():
        start = 0
        for group in groups:
            keys[start : start + group.shape[0], :] = group[...]
            start += group.shape[0]

    factor = QK ** (-0.5) * float(np.log2(np.e))
    offset = lax.axis_index("head") * rows

    def score_rows(i):
        return lax.dot_general(
            query_rows[i * part : (i + 1) * part, :],
            keys[...],
            (((1,), (1,)), ((), ())),
            preferred_element_type=jnp.float32,
        )

    def finish(i, score):
        query_pos = offset + lax.rem(lax.broadcasted_iota(jnp.int32, (part, own), 0), rows)
        key_pos = lax.broadcasted_iota(jnp.int32, (part, own), 1)
        diagonal = jnp.where(key_pos <= query_pos, score[:, :own], HIDDEN)
        score = jnp.concatenate([diagonal, score[:, own:]], 1)
        peak = jnp.max(score, axis=-1, keepdims=True)
        probs = jnp.exp2((score - peak) * factor)
        totals = jnp.sum(probs, axis=-1, keepdims=True)
        sums = jnp.dot(
            probs.astype(jnp.bfloat16), keys[:, :KV], preferred_element_type=jnp.float32
        )
        latent_out = (sums / totals).astype(jnp.bfloat16)
        for j in range(part // rows):
            head = i * (part // rows) + j
            piece = jnp.dot(
                latent_out[j * rows : (j + 1) * rows],
                value_up[head],
                preferred_element_type=jnp.float32,
            )
            out[:, head * VD : (head + 1) * VD] = piece.astype(jnp.bfloat16)

    count = total // part
    score = score_rows(0)
    for i in range(count):
        later = score_rows(i + 1) if i + 1 < count else None
        finish(i, score)
        score = later


def attend(query_rows, value_up, keys, rows):
    heads = value_up.shape[0]
    step = 8
    steps = heads // step
    key_total = sum(key.shape[0] for key in keys)
    return pl.pallas_call(
        functools.partial(attend_kernel, 4 * rows, len(keys)),
        grid=(steps,),
        in_specs=[
            pl.BlockSpec((step * rows, WIDE), lambda i: (i, 0)),
            pl.BlockSpec((step, KV, VD), lambda i: (i, 0, 0)),
        ]
        + [pl.BlockSpec(key.shape, lambda i: (0, 0)) for key in keys],
        out_specs=pl.BlockSpec((rows, step * VD), lambda i: (0, i)),
        out_shape=jax.ShapeDtypeStruct((rows, heads * VD), jnp.bfloat16),
        scratch_shapes=[pltpu.VMEM((key_total, WIDE), jnp.bfloat16)],
        cost_estimate=pl.CostEstimate(
            flops=2 * heads * rows * (key_total * (WIDE + KV) + KV * VD),
            bytes_accessed=2 * heads * (KV * VD + rows * (WIDE + VD)) + 2 * key_total * WIDE,
            transcendentals=heads * rows * key_total,
        ),
        compiler_params=pltpu.CompilerParams(
            vmem_limit_bytes=(12 << 20) + 16 * key_total * WIDE
        ),
        name="attend",
    )(query_rows, value_up, *keys)


def project_kernel(count, offsets, *refs):
    pieces = len(offsets)
    firsts, seconds = refs[:pieces], refs[pieces : 2 * pieces]
    own_weight, other_weight = refs[2 * pieces : 2 * pieces + 2]
    out, held, sems = refs[-3:]
    rows = firsts[0].shape[0]

    def stack(parts):
        return jnp.concatenate([part[...] for part in parts], 0) if pieces > 1 else parts[0][...]

    product = jnp.dot(stack(firsts), own_weight[...], preferred_element_type=jnp.float32)
    product += jnp.dot(stack(seconds), other_weight[...], preferred_element_type=jnp.float32)
    held[...] = product.astype(jnp.bfloat16)
    block = lax.axis_index("seq")
    half = block // 2
    place = jnp.where(block - 2 * half == 0, half, count - 1 - half)
    copies = []
    for i, offset in enumerate(offsets):
        at = lax.rem(place + offset % count, count)
        source = jnp.where(at < count // 2, 2 * at, 2 * (count - 1 - at) + 1)
        copies.append(
            pltpu.make_async_copy(held.at[pl.ds(i * rows, rows), :], out.at[source, 0], sems.at[i])
        )
        copies[-1].start()
    for copy in copies:
        copy.wait()


def project(count, offsets, firsts, seconds, own_weight, other_weight, mixed):
    rows, depth = firsts[0].shape
    columns = own_weight.shape[1]
    pieces = len(offsets)
    operands = [*firsts, *seconds, own_weight, other_weight]
    aliases = {}
    if mixed is not None:
        aliases = {len(operands): 0}
        operands.append(mixed)
    vmem = pl.BlockSpec(memory_space=pltpu.VMEM)
    anywhere = pl.BlockSpec(memory_space=pl.ANY)
    return pl.pallas_call(
        functools.partial(project_kernel, count, offsets),
        in_specs=[vmem] * (2 * pieces + 2) + [anywhere] * len(aliases),
        out_specs=anywhere,
        out_shape=jax.ShapeDtypeStruct((count, 1, rows, columns), jnp.bfloat16),
        scratch_shapes=[
            pltpu.VMEM((pieces * rows, columns), jnp.bfloat16),
            pltpu.SemaphoreType.DMA((pieces,)),
        ],
        input_output_aliases=aliases,
        compiler_params=pltpu.CompilerParams(vmem_limit_bytes=8 << 20),
        cost_estimate=pl.CostEstimate(
            flops=4 * pieces * rows * depth * columns,
            bytes_accessed=4 * depth * columns,
            transcendentals=0,
        ),
        name="project",
    )(*operands)


def gather_plan(count):
    moves = []
    bit = count // 2
    slots = [0]
    while bit:
        moves += [(slot, bit) for slot in slots]
        slots += [slot | bit for slot in slots]
        bit //= 2
    return moves


def layer(queries, latents, latent_gain, key_up, value_up, out_weight):
    seq_count = lax.axis_size("seq")
    head_count = lax.axis_size("head")
    rows = queries.shape[0]
    swap_pairs = [(i, (i + 1) % head_count) for i in range(head_count)]
    everyone = range(seq_count)

    own_keys, half_keys = prepare(latents.T, latent_gain.reshape(1, KV))
    slots = {0: half_keys}
    for slot, bit in gather_plan(seq_count):
        slots[slot | bit] = lax.ppermute(slots[slot], "seq", [(d ^ bit, d) for d in everyone])
    near = [m for m in range(1, seq_count) if m % 2 == 0] + [1]
    far = [m for m in range(2, seq_count) if m % 2 == 1]
    near_keys = jnp.concatenate([slots[m] for m in near], 0)
    far_keys = jnp.concatenate([slots[m] for m in far], 0)
    near_swap = lax.ppermute(near_keys, "head", swap_pairs)
    far_swap = lax.ppermute(far_keys, "head", swap_pairs)
    keys = [own_keys, near_keys, far_keys, near_swap, far_swap]

    key_other = lax.ppermute(key_up, "head", swap_pairs)
    value_other = lax.ppermute(value_up, "head", swap_pairs)
    weight_other = lax.ppermute(out_weight, "head", swap_pairs)
    rows_a = lift(queries, key_up, False)
    heads_a = attend(rows_a, value_up, keys, rows)
    rows_b = lift(queries, key_other, True)
    heads_b = attend(rows_b, value_other, keys, rows)

    order = list(range(0, seq_count, 2)) + list(range(seq_count - 1, 0, -2))
    right = [(order[i], order[(i + 1) % seq_count]) for i in everyone]
    left = [(b, a) for a, b in right]
    steps = seq_count // 2

    def put(mixed, *pieces):
        firsts, seconds, offsets = zip(*pieces)
        return project(
            seq_count, offsets, firsts, seconds, out_weight, weight_other, mixed
        )

    right_a, right_b, left_a, left_b = heads_a, heads_b, heads_a, heads_b
    mixed = put(None, (heads_a, heads_b, 0))
    for step in range(1, steps + 1):
        last = step == steps
        right_a = lax.ppermute(right_a, "seq", right)
        if not last:
            left_a = lax.ppermute(left_a, "seq", left)
            right_b = lax.ppermute(right_b, "seq", right)
        left_b = lax.ppermute(left_b, "seq", left)
        if last:
            mixed = put(mixed, (right_a, left_b, step))
        else:
            mixed = put(mixed, (right_a, right_b, -step), (left_a, left_b, step))
    return mixed


def solution(mesh):
    placed = (
        P(("groups", "seq", "head"), None),
        P(("groups", "seq"), None),
        P(),
        P("head", None, None),
        P("head", None, None),
        P("head", "seq"),
    )
    return jax.shard_map(
        layer,
        mesh=mesh,
        in_specs=placed,
        out_specs=P("groups", "head", None, "seq"),
        check_vma=False,
    )
```

```python
import functools

import jax
import jax.numpy as jnp
import numpy as np
from jax import lax
from jax.experimental import pallas as pl
from jax.experimental.pallas import tpu as pltpu
from jax.sharding import PartitionSpec as P


KV = 512
ROPE = 64
NOPE = 128
VD = 128
QK = NOPE + ROPE
WIDE = KV + 2 * ROPE
EPS = 1e-06
HIDDEN = -1e30


def rope_angles(position, index):
    middle = ROPE // 2
    frequency = jnp.ones(index.shape, jnp.float32)
    for bit in range(middle.bit_length() - 1):
        factor = float(10000.0 ** (-(1 << bit) / middle))
        frequency *= jnp.where((index >> bit) % 2 == 1, factor, 1.0)
    return position.astype(jnp.float32) * frequency


def tag_lanes(rows, value):
    lane = lax.broadcasted_iota(jnp.int32, (rows, ROPE), 1)
    return value(lane).astype(jnp.bfloat16)


def prepare_kernel(half, latents, gain, full_out, half_out):
    block = lax.axis_index("seq")
    latent_f = latents[...].astype(jnp.float32)
    tokens = latent_f.shape[1]
    compressed = latent_f[:KV]
    spread = jnp.mean(compressed * compressed, axis=0, keepdims=True)
    normed = (compressed * lax.rsqrt(spread + EPS)).T * gain[...]
    full_out[:, :KV] = normed.astype(jnp.bfloat16)
    shape = (ROPE // 2, tokens)
    position = block * tokens + lax.broadcasted_iota(jnp.int32, shape, 1)
    angles = rope_angles(position, lax.broadcasted_iota(jnp.int32, shape, 0))
    cosine, sine = jnp.cos(angles), jnp.sin(angles)
    former, latter = latent_f[KV : KV + ROPE // 2], latent_f[KV + ROPE // 2 :]
    halves = [former * cosine - latter * sine, former * sine + latter * cosine]
    rope = jnp.concatenate(halves, 0).T.astype(jnp.bfloat16)
    tags = tag_lanes(tokens, lambda lane: jnp.where(lane == block, 1.0, 0.0))
    full_out[:, KV:] = jnp.concatenate([rope, tags], -1)
    start = lax.axis_index("head") * half
    half_out[...] = full_out[pl.ds(pl.multiple_of(start, half), half), :]


def prepare(latents, gain):
    rows = latents.shape[1]
    half = rows // 2
    return pl.pallas_call(
        functools.partial(prepare_kernel, half),
        out_shape=[
            jax.ShapeDtypeStruct((rows, WIDE), jnp.bfloat16),
            jax.ShapeDtypeStruct((half, WIDE), jnp.bfloat16),
        ],
        compiler_params=pltpu.CompilerParams(vmem_limit_bytes=12 << 20),
        cost_estimate=pl.CostEstimate(
            flops=10**8, bytes_accessed=4 * rows * WIDE, transcendentals=rows
        ),
        name="prepare",
    )(latents, gain)


def lift_kernel(queries, key_up, out):
    rows = queries.shape[0]
    heads = key_up.shape[0]
    block = lax.axis_index("seq")
    for head in range(heads):
        plain = queries[:, head * QK : head * QK + NOPE]
        lifted = jnp.dot(plain, key_up[head], preferred_element_type=jnp.float32)
        out[pl.ds(head * rows, rows), :KV] = lifted.astype(jnp.bfloat16)
    shape = (rows, ROPE)
    first = (2 * block + lax.axis_index("head")) * rows
    position = first + lax.broadcasted_iota(jnp.int32, shape, 0)
    lane = lax.broadcasted_iota(jnp.int32, shape, 1)
    upper = lane >= ROPE // 2
    angles = rope_angles(position, jnp.where(upper, lane - ROPE // 2, lane))
    cosine = jnp.concatenate([jnp.cos(angles)] * heads, 0)
    sine = jnp.sin(angles)
    sine = jnp.concatenate([jnp.where(upper, sine, -sine)] * heads, 0)
    turning = jnp.concatenate(
        [
            queries[:, head * QK + NOPE : (head + 1) * QK].astype(jnp.float32)
            for head in range(heads)
        ],
        0,
    )
    swapped = jnp.concatenate([turning[:, ROPE // 2 :], turning[:, : ROPE // 2]], -1)
    turned = (turning * cosine + swapped * sine).astype(jnp.bfloat16)
    tags = tag_lanes(heads * rows, lambda lane: jnp.where(lane > block, HIDDEN, 0.0))
    out[:, KV:] = jnp.concatenate([turned, tags], -1)


def lift(queries, key_up, other):
    rows = queries.shape[0]
    heads = key_up.shape[0]
    step = 8
    steps = heads // step

    def query_block(i):
        half = lax.axis_index("head")
        return (0, (1 - half if other else half) * steps + i)

    return pl.pallas_call(
        lift_kernel,
        grid=(steps,),
        in_specs=[
            pl.BlockSpec((rows, step * QK), query_block),
            pl.BlockSpec((step, NOPE, KV), lambda i: (i, 0, 0)),
        ],
        out_specs=pl.BlockSpec((step * rows, WIDE), lambda i: (i, 0)),
        out_shape=jax.ShapeDtypeStruct((heads * rows, WIDE), jnp.bfloat16),
        cost_estimate=pl.CostEstimate(
            flops=2 * heads * rows * NOPE * KV,
            bytes_accessed=2 * heads * (NOPE * KV + rows * (QK + WIDE)),
            transcendentals=0,
        ),
        compiler_params=pltpu.CompilerParams(vmem_limit_bytes=12 << 20),
        name="lift",
    )(queries, key_up)


def attend_kernel(part, groups, query_rows, value_up, *rest):
    groups, (out, keys) = rest[:groups], rest[groups:]
    total = query_rows.shape[0]
    heads = value_up.shape[0]
    rows = total // heads
    own = groups[0].shape[0]

    @pl.when(pl.program_id(0) == 0)
    def _():
        start = 0
        for group in groups:
            keys[start : start + group.shape[0], :] = group[...]
            start += group.shape[0]

    factor = QK ** (-0.5) * float(np.log2(np.e))
    offset = lax.axis_index("head") * rows

    def score_rows(i):
        return lax.dot_general(
            query_rows[i * part : (i + 1) * part, :],
            keys[...],
            (((1,), (1,)), ((), ())),
            preferred_element_type=jnp.float32,
        )

    def finish(i, score):
        query_pos = offset + lax.rem(lax.broadcasted_iota(jnp.int32, (part, own), 0), rows)
        key_pos = lax.broadcasted_iota(jnp.int32, (part, own), 1)
        diagonal = jnp.where(key_pos <= query_pos, score[:, :own], HIDDEN)
        score = jnp.concatenate([diagonal, score[:, own:]], 1)
        peak = jnp.max(score, axis=-1, keepdims=True)
        probs = jnp.exp2((score - peak) * factor)
        totals = jnp.sum(probs, axis=-1, keepdims=True)
        sums = jnp.dot(
            probs.astype(jnp.bfloat16), keys[:, :KV], preferred_element_type=jnp.float32
        )
        latent_out = (sums / totals).astype(jnp.bfloat16)
        for j in range(part // rows):
            head = i * (part // rows) + j
            piece = jnp.dot(
                latent_out[j * rows : (j + 1) * rows],
                value_up[head],
                preferred_element_type=jnp.float32,
            )
            out[:, head * VD : (head + 1) * VD] = piece.astype(jnp.bfloat16)

    count = total // part
    score = score_rows(0)
    for i in range(count):
        later = score_rows(i + 1) if i + 1 < count else None
        finish(i, score)
        score = later


def attend(query_rows, value_up, keys, rows, blocks):
    step = 8
    first, count = blocks
    heads = count * step
    key_total = sum(key.shape[0] for key in keys)
    return pl.pallas_call(
        functools.partial(attend_kernel, 4 * rows, len(keys)),
        grid=(count,),
        in_specs=[
            pl.BlockSpec((step * rows, WIDE), lambda i: (first + i, 0)),
            pl.BlockSpec((step, KV, VD), lambda i: (first + i, 0, 0)),
        ]
        + [pl.BlockSpec(key.shape, lambda i: (0, 0)) for key in keys],
        out_specs=pl.BlockSpec((rows, step * VD), lambda i: (0, i)),
        out_shape=jax.ShapeDtypeStruct((rows, heads * VD), jnp.bfloat16),
        scratch_shapes=[pltpu.VMEM((key_total, WIDE), jnp.bfloat16)],
        cost_estimate=pl.CostEstimate(
            flops=2 * heads * rows * (key_total * (WIDE + KV) + KV * VD),
            bytes_accessed=2 * heads * (KV * VD + rows * (WIDE + VD)) + 2 * key_total * WIDE,
            transcendentals=heads * rows * key_total,
        ),
        compiler_params=pltpu.CompilerParams(
            vmem_limit_bytes=(12 << 20) + 16 * key_total * WIDE
        ),
        name="attend",
    )(query_rows, value_up, *keys)


def project_kernel(count, offsets, chunks, *refs):
    pieces = len(offsets)
    parts = refs[: pieces * chunks]
    own_weight, other_weight = refs[pieces * chunks : pieces * chunks + 2]
    out, held, sems = refs[-3:]
    rows = parts[0].shape[0]
    product = None
    start = 0
    for chunk in range(chunks):
        stack = [parts[piece * chunks + chunk][...] for piece in range(pieces)]
        stack = jnp.concatenate(stack, 0) if pieces > 1 else stack[0]
        depth = stack.shape[1]
        if start < own_weight.shape[0]:
            weight = own_weight[start : start + depth, :]
        else:
            weight = other_weight[...]
        start += depth
        part = jnp.dot(stack, weight, preferred_element_type=jnp.float32)
        product = part if product is None else product + part
    held[...] = product.astype(jnp.bfloat16)
    block = lax.axis_index("seq")
    half = block // 2
    place = jnp.where(block - 2 * half == 0, half, count - 1 - half)
    copies = []
    for i, offset in enumerate(offsets):
        at = lax.rem(place + offset % count, count)
        source = jnp.where(at < count // 2, 2 * at, 2 * (count - 1 - at) + 1)
        copies.append(
            pltpu.make_async_copy(held.at[pl.ds(i * rows, rows), :], out.at[source, 0], sems.at[i])
        )
        copies[-1].start()
    for copy in copies:
        copy.wait()


def project(count, pieces, own_weight, other_weight, mixed):
    offsets = [offset for offset, _ in pieces]
    operands = [part for _, parts in pieces for part in parts]
    chunks = len(operands) // len(pieces)
    rows = operands[0].shape[0]
    depth, columns = own_weight.shape
    operands += [own_weight, other_weight]
    aliases = {}
    vmem = pl.BlockSpec(memory_space=pltpu.VMEM)
    anywhere = pl.BlockSpec(memory_space=pl.ANY)
    specs = [vmem] * len(operands)
    if mixed is not None:
        aliases = {len(operands): 0}
        operands.append(mixed)
        specs.append(anywhere)
    return pl.pallas_call(
        functools.partial(project_kernel, count, offsets, chunks),
        in_specs=specs,
        out_specs=anywhere,
        out_shape=jax.ShapeDtypeStruct((count, 1, rows, columns), jnp.bfloat16),
        scratch_shapes=[
            pltpu.VMEM((len(pieces) * rows, columns), jnp.bfloat16),
            pltpu.SemaphoreType.DMA((len(pieces),)),
        ],
        input_output_aliases=aliases,
        compiler_params=pltpu.CompilerParams(vmem_limit_bytes=8 << 20),
        cost_estimate=pl.CostEstimate(
            flops=4 * len(pieces) * rows * depth * columns,
            bytes_accessed=4 * depth * columns,
            transcendentals=0,
        ),
        name="project",
    )(*operands)


def touch_kernel(value, out):
    out[...] = jnp.zeros_like(out)


def touch(value):
    return pl.pallas_call(
        touch_kernel,
        in_specs=[pl.BlockSpec(memory_space=pltpu.VMEM)],
        out_shape=jax.ShapeDtypeStruct((8, 128), jnp.float32),
        compiler_params=pltpu.CompilerParams(vmem_limit_bytes=8 << 20, has_side_effects=True),
        name="touch",
    )(value)


def gather_plan(count):
    moves = []
    bit = count // 2
    slots = [0]
    while bit:
        moves += [(slot, bit) for slot in slots]
        slots += [slot | bit for slot in slots]
        bit //= 2
    return moves


def ring_order(steps):
    right = ["a1", "b1", "a2", "c1"]
    left = ["a1", "b1", "a2", "c1"]
    for step in range(2, steps - 1):
        right += [f"b{step}", f"c{step}", f"a{step + 1}"]
        left += [f"b{step}", f"a{step + 1}", f"c{step}"]
    step = steps - 1
    right += [f"c{step}", f"b{step}", f"c{steps}"]
    left += [f"b{step}", f"a{steps}", f"c{step}", f"b{steps}"]
    names = []
    for i in range(len(left)):
        names += ["r" + right[i]] if i < len(right) else []
        names.append("l" + left[i])
    return names


def send(value, axis, pairs):
    return lax.ppermute(value, axis, pairs)


def layer(queries, latents, latent_gain, key_up, value_up, out_weight):
    seq_count = lax.axis_size("seq")
    head_count = lax.axis_size("head")
    rows = queries.shape[0]
    swap_pairs = [(i, (i + 1) % head_count) for i in range(head_count)]
    everyone = range(seq_count)

    own_keys, half_keys = prepare(latents.T, latent_gain.reshape(1, KV))
    slots = {0: half_keys}
    for slot, bit in gather_plan(seq_count):
        slots[slot | bit] = send(slots[slot], "seq", [(d ^ bit, d) for d in everyone])
    near = [m for m in range(1, seq_count) if m % 2 == 0] + [1]
    far = [m for m in range(2, seq_count) if m % 2 == 1]
    near_keys = jnp.concatenate([slots[m] for m in near], 0)
    far_keys = jnp.concatenate([slots[m] for m in far], 0)
    near_swap = send(near_keys, "head", swap_pairs)
    far_swap = send(far_keys, "head", swap_pairs)
    keys = [own_keys, near_keys, far_keys, near_swap, far_swap]

    key_other = send(key_up, "head", swap_pairs)
    value_other = send(value_up, "head", swap_pairs)
    weight_other = send(out_weight, "head", swap_pairs)
    rows_a = lift(queries, key_up, False)
    touch(value_up)
    rows_b = lift(queries, key_other, True)
    blocks = key_up.shape[0] // 8
    first = blocks // 2
    chunks = {}
    chunks["a"] = attend(rows_a, value_up, keys, rows, (0, first))
    chunks["b"] = attend(rows_a, value_up, keys, rows, (first, blocks - first))
    chunks["c"] = attend(rows_b, value_other, keys, rows, (0, blocks))

    order = list(range(0, seq_count, 2)) + list(range(seq_count - 1, 0, -2))
    right = [(order[i], order[(i + 1) % seq_count]) for i in everyone]
    left = [(b, a) for a, b in right]
    steps = seq_count // 2
    held = {way + chunk + "0": value for chunk, value in chunks.items() for way in "rl"}
    for step in range(1, steps + 1):
        for name in ring_order(steps):
            if name[2:] == str(step):
                value = held[name[:2] + str(step - 1)]
                held[name] = send(value, "seq", right if name[0] == "r" else left)

    def put(mixed, *pieces):
        return project(seq_count, pieces, out_weight, weight_other, mixed)

    def from_way(way, step):
        return [held[f"{way}{chunk}{step}"] for chunk in "abc"]

    mixed = put(None, (0, from_way("r", 0)))
    for step in range(1, steps - 1):
        mixed = put(mixed, (-step, from_way("r", step)), (step, from_way("l", step)))
    step = steps - 1
    mixed = put(mixed, (-step, from_way("r", step)))
    mixed = put(mixed, (step, from_way("l", step)))
    final = [held[f"la{steps}"], held[f"lb{steps}"], held[f"rc{steps}"]]
    return put(mixed, (steps, final))


def solution(mesh):
    placed = (
        P(("groups", "seq", "head"), None),
        P(("groups", "seq"), None),
        P(),
        P("head", None, None),
        P("head", None, None),
        P("head", "seq"),
    )
    return jax.shard_map(
        layer,
        mesh=mesh,
        in_specs=placed,
        out_specs=P("groups", "head", None, "seq"),
        check_vma=False,
    )
```

```python
import functools

import jax
import jax.numpy as jnp
import numpy as np
from jax import lax
from jax.experimental import pallas as pl
from jax.experimental.pallas import tpu as pltpu
from jax.sharding import PartitionSpec as P


KV = 512
ROPE = 64
NOPE = 128
VD = 128
QK = NOPE + ROPE
WIDE = KV + 2 * ROPE
EPS = 1e-06
HIDDEN = -1e30


def rope_angles(position, index):
    middle = ROPE // 2
    frequency = jnp.ones(index.shape, jnp.float32)
    for bit in range(middle.bit_length() - 1):
        factor = float(10000.0 ** (-(1 << bit) / middle))
        frequency *= jnp.where((index >> bit) % 2 == 1, factor, 1.0)
    return position.astype(jnp.float32) * frequency


def tag_lanes(rows, value):
    lane = lax.broadcasted_iota(jnp.int32, (rows, ROPE), 1)
    return value(lane).astype(jnp.bfloat16)


def prepare_kernel(half, latents, gain, full_out, half_out):
    block = lax.axis_index("seq")
    latent_f = latents[...].astype(jnp.float32)
    tokens = latent_f.shape[1]
    compressed = latent_f[:KV]
    spread = jnp.mean(compressed * compressed, axis=0, keepdims=True)
    normed = (compressed * lax.rsqrt(spread + EPS)).T * gain[...]
    full_out[:, :KV] = normed.astype(jnp.bfloat16)
    shape = (ROPE // 2, tokens)
    position = block * tokens + lax.broadcasted_iota(jnp.int32, shape, 1)
    angles = rope_angles(position, lax.broadcasted_iota(jnp.int32, shape, 0))
    cosine, sine = jnp.cos(angles), jnp.sin(angles)
    former, latter = latent_f[KV : KV + ROPE // 2], latent_f[KV + ROPE // 2 :]
    halves = [former * cosine - latter * sine, former * sine + latter * cosine]
    rope = jnp.concatenate(halves, 0).T.astype(jnp.bfloat16)
    tags = tag_lanes(tokens, lambda lane: jnp.where(lane == block, 1.0, 0.0))
    full_out[:, KV:] = jnp.concatenate([rope, tags], -1)
    start = lax.axis_index("head") * half
    half_out[...] = full_out[pl.ds(pl.multiple_of(start, half), half), :]


def prepare(latents, gain):
    rows = latents.shape[1]
    half = rows // 2
    return pl.pallas_call(
        functools.partial(prepare_kernel, half),
        out_shape=[
            jax.ShapeDtypeStruct((rows, WIDE), jnp.bfloat16),
            jax.ShapeDtypeStruct((half, WIDE), jnp.bfloat16),
        ],
        compiler_params=pltpu.CompilerParams(vmem_limit_bytes=12 << 20),
        cost_estimate=pl.CostEstimate(
            flops=10**8, bytes_accessed=4 * rows * WIDE, transcendentals=rows
        ),
        name="prepare",
    )(latents, gain)


def lift_kernel(queries, key_up, out):
    rows = queries.shape[0]
    heads = key_up.shape[0]
    block = lax.axis_index("seq")
    for head in range(heads):
        plain = queries[:, head * QK : head * QK + NOPE]
        lifted = jnp.dot(plain, key_up[head], preferred_element_type=jnp.float32)
        out[pl.ds(head * rows, rows), :KV] = lifted.astype(jnp.bfloat16)
    shape = (rows, ROPE)
    first = (2 * block + lax.axis_index("head")) * rows
    position = first + lax.broadcasted_iota(jnp.int32, shape, 0)
    lane = lax.broadcasted_iota(jnp.int32, shape, 1)
    upper = lane >= ROPE // 2
    angles = rope_angles(position, jnp.where(upper, lane - ROPE // 2, lane))
    cosine = jnp.concatenate([jnp.cos(angles)] * heads, 0)
    sine = jnp.sin(angles)
    sine = jnp.concatenate([jnp.where(upper, sine, -sine)] * heads, 0)
    turning = jnp.concatenate(
        [
            queries[:, head * QK + NOPE : (head + 1) * QK].astype(jnp.float32)
            for head in range(heads)
        ],
        0,
    )
    swapped = jnp.concatenate([turning[:, ROPE // 2 :], turning[:, : ROPE // 2]], -1)
    turned = (turning * cosine + swapped * sine).astype(jnp.bfloat16)
    tags = tag_lanes(heads * rows, lambda lane: jnp.where(lane > block, HIDDEN, 0.0))
    out[:, KV:] = jnp.concatenate([turned, tags], -1)


def lift(queries, key_up, other):
    rows = queries.shape[0]
    heads = key_up.shape[0]
    step = 8
    steps = heads // step

    def query_block(i):
        half = lax.axis_index("head")
        return (0, (1 - half if other else half) * steps + i)

    return pl.pallas_call(
        lift_kernel,
        grid=(steps,),
        in_specs=[
            pl.BlockSpec((rows, step * QK), query_block),
            pl.BlockSpec((step, NOPE, KV), lambda i: (i, 0, 0)),
        ],
        out_specs=pl.BlockSpec((step * rows, WIDE), lambda i: (i, 0)),
        out_shape=jax.ShapeDtypeStruct((heads * rows, WIDE), jnp.bfloat16),
        cost_estimate=pl.CostEstimate(
            flops=2 * heads * rows * NOPE * KV,
            bytes_accessed=2 * heads * (NOPE * KV + rows * (QK + WIDE)),
            transcendentals=0,
        ),
        compiler_params=pltpu.CompilerParams(vmem_limit_bytes=12 << 20),
        name="lift",
    )(queries, key_up)


def attend_kernel(part, groups, query_rows, value_up, *rest):
    groups, (out, keys) = rest[:groups], rest[groups:]
    total = query_rows.shape[0]
    heads = value_up.shape[0]
    rows = total // heads
    own = groups[0].shape[0]

    @pl.when(pl.program_id(0) == 0)
    def _():
        start = 0
        for group in groups:
            keys[start : start + group.shape[0], :] = group[...]
            start += group.shape[0]

    factor = QK ** (-0.5) * float(np.log2(np.e))
    offset = lax.axis_index("head") * rows

    def score_rows(i):
        return lax.dot_general(
            query_rows[i * part : (i + 1) * part, :],
            keys[...],
            (((1,), (1,)), ((), ())),
            preferred_element_type=jnp.float32,
        )

    def finish(i, score):
        query_pos = offset + lax.rem(lax.broadcasted_iota(jnp.int32, (part, own), 0), rows)
        key_pos = lax.broadcasted_iota(jnp.int32, (part, own), 1)
        diagonal = jnp.where(key_pos <= query_pos, score[:, :own], HIDDEN)
        score = jnp.concatenate([diagonal, score[:, own:]], 1)
        peak = jnp.max(score, axis=-1, keepdims=True)
        probs = jnp.exp2((score - peak) * factor)
        totals = jnp.sum(probs, axis=-1, keepdims=True)
        sums = jnp.dot(
            probs.astype(jnp.bfloat16), keys[:, :KV], preferred_element_type=jnp.float32
        )
        latent_out = (sums / totals).astype(jnp.bfloat16)
        for j in range(part // rows):
            head = i * (part // rows) + j
            piece = jnp.dot(
                latent_out[j * rows : (j + 1) * rows],
                value_up[head],
                preferred_element_type=jnp.float32,
            )
            out[:, head * VD : (head + 1) * VD] = piece.astype(jnp.bfloat16)

    count = total // part
    score = score_rows(0)
    for i in range(count):
        later = score_rows(i + 1) if i + 1 < count else None
        finish(i, score)
        score = later


def attend(query_rows, value_up, keys, rows, blocks):
    step = 8
    first, count = blocks
    heads = count * step
    key_total = sum(key.shape[0] for key in keys)
    return pl.pallas_call(
        functools.partial(attend_kernel, 4 * rows, len(keys)),
        grid=(count,),
        in_specs=[
            pl.BlockSpec((step * rows, WIDE), lambda i: (first + i, 0)),
            pl.BlockSpec((step, KV, VD), lambda i: (first + i, 0, 0)),
        ]
        + [pl.BlockSpec(key.shape, lambda i: (0, 0)) for key in keys],
        out_specs=pl.BlockSpec((rows, step * VD), lambda i: (0, i)),
        out_shape=jax.ShapeDtypeStruct((rows, heads * VD), jnp.bfloat16),
        scratch_shapes=[pltpu.VMEM((key_total, WIDE), jnp.bfloat16)],
        cost_estimate=pl.CostEstimate(
            flops=2 * heads * rows * (key_total * (WIDE + KV) + KV * VD),
            bytes_accessed=2 * heads * (KV * VD + rows * (WIDE + VD)) + 2 * key_total * WIDE,
            transcendentals=heads * rows * key_total,
        ),
        compiler_params=pltpu.CompilerParams(
            vmem_limit_bytes=(12 << 20) + 16 * key_total * WIDE
        ),
        name="attend",
    )(query_rows, value_up, *keys)


def project_kernel(count, offsets, rows_of, finish, added, *refs):
    pieces, chunks = len(offsets), len(rows_of)
    parts = refs[: pieces * chunks]
    weight = refs[pieces * chunks]
    product = None
    for chunk, start in enumerate(rows_of):
        stack = [parts[piece * chunks + chunk][...] for piece in range(pieces)]
        stack = jnp.concatenate(stack, 0) if pieces > 1 else stack[0]
        part = jnp.dot(
            stack,
            weight[start : start + stack.shape[1], :],
            preferred_element_type=jnp.float32,
        )
        product = part if product is None else product + part
    if added:
        product += refs[pieces * chunks + 1][...]
    if not finish:
        refs[-1][...] = product
        return
    out, held, sems = refs[-3:]
    rows = parts[0].shape[0]
    held[...] = product.astype(jnp.bfloat16)
    block = lax.axis_index("seq")
    half = block // 2
    place = jnp.where(block - 2 * half == 0, half, count - 1 - half)
    copies = []
    for i, offset in enumerate(offsets):
        at = lax.rem(place + offset % count, count)
        source = jnp.where(at < count // 2, 2 * at, 2 * (count - 1 - at) + 1)
        copies.append(
            pltpu.make_async_copy(held.at[pl.ds(i * rows, rows), :], out.at[source, 0], sems.at[i])
        )
        copies[-1].start()
    for copy in copies:
        copy.wait()


def project(count, pieces, rows_of, weight, earlier=None, mixed=None, finish=True):
    offsets = [offset for offset, _ in pieces]
    operands = [part for _, parts in pieces for part in parts]
    rows = operands[0].shape[0]
    columns = weight.shape[1]
    total = len(pieces) * rows
    operands.append(weight)
    if earlier is not None:
        operands.append(earlier)
    aliases = {}
    vmem = pl.BlockSpec(memory_space=pltpu.VMEM)
    anywhere = pl.BlockSpec(memory_space=pl.ANY)
    specs = [vmem] * len(operands)
    if finish and mixed is not None:
        aliases = {len(operands): 0}
        operands.append(mixed)
        specs.append(anywhere)
    if finish:
        shape = jax.ShapeDtypeStruct((count, 1, rows, columns), jnp.bfloat16)
        scratch = [
            pltpu.VMEM((total, columns), jnp.bfloat16),
            pltpu.SemaphoreType.DMA((len(pieces),)),
        ]
    else:
        shape = jax.ShapeDtypeStruct((total, columns), jnp.float32)
        scratch = []
    return pl.pallas_call(
        functools.partial(
            project_kernel, count, offsets, rows_of, finish, earlier is not None
        ),
        in_specs=specs,
        out_specs=anywhere if finish else vmem,
        out_shape=shape,
        scratch_shapes=scratch,
        input_output_aliases=aliases,
        compiler_params=pltpu.CompilerParams(vmem_limit_bytes=8 << 20),
        cost_estimate=pl.CostEstimate(
            flops=2 * total * weight.shape[0] * columns,
            bytes_accessed=2 * weight.shape[0] * columns,
            transcendentals=0,
        ),
        name="project",
    )(*operands)


def touch_kernel(value, out):
    out[...] = jnp.zeros_like(out)


def touch(value):
    return pl.pallas_call(
        touch_kernel,
        in_specs=[pl.BlockSpec(memory_space=pltpu.VMEM)],
        out_shape=jax.ShapeDtypeStruct((8, 128), jnp.float32),
        compiler_params=pltpu.CompilerParams(vmem_limit_bytes=8 << 20, has_side_effects=True),
        name="touch",
    )(value)


def gather_plan(count):
    moves = []
    bit = count // 2
    slots = [0]
    while bit:
        moves += [(slot, bit) for slot in slots]
        slots += [slot | bit for slot in slots]
        bit //= 2
    return moves


def ring_order(steps):
    return [
        way + chunk + str(step) for step in range(1, steps + 1) for chunk in "ab" for way in "rl"
    ]


def layer(queries, latents, latent_gain, key_up, value_up, out_weight):
    seq_count = lax.axis_size("seq")
    head_count = lax.axis_size("head")
    rows = queries.shape[0]
    swap_pairs = [(i, (i + 1) % head_count) for i in range(head_count)]
    everyone = range(seq_count)

    own_keys, half_keys = prepare(latents.T, latent_gain.reshape(1, KV))
    slots = {0: half_keys}
    for slot, bit in gather_plan(seq_count):
        slots[slot | bit] = lax.ppermute(slots[slot], "seq", [(d ^ bit, d) for d in everyone])
    near = [m for m in range(1, seq_count) if m % 2 == 0] + [1]
    far = [m for m in range(2, seq_count) if m % 2 == 1]
    near_keys = jnp.concatenate([slots[m] for m in near], 0)
    far_keys = jnp.concatenate([slots[m] for m in far], 0)
    near_swap = lax.ppermute(near_keys, "head", swap_pairs)
    far_swap = lax.ppermute(far_keys, "head", swap_pairs)
    keys = [own_keys, near_keys, far_keys, near_swap, far_swap]

    key_other = lax.ppermute(key_up, "head", swap_pairs)
    value_other = lax.ppermute(value_up, "head", swap_pairs)
    weight_other = lax.ppermute(out_weight, "head", swap_pairs)
    rows_a = lift(queries, key_up, False)
    touch(value_up)
    rows_b = lift(queries, key_other, True)
    blocks = (0, key_up.shape[0] // 8)
    chunks = {}
    chunks["a"] = attend(rows_a, value_up, keys, rows, blocks)
    chunks["b"] = attend(rows_b, value_other, keys, rows, blocks)

    order = list(range(0, seq_count, 2)) + list(range(seq_count - 1, 0, -2))
    right = [(order[i], order[(i + 1) % seq_count]) for i in everyone]
    left = [(b, a) for a, b in right]
    steps = seq_count // 2
    held = {way + chunk + "0": value for chunk, value in chunks.items() for way in "rl"}
    middle = chunks["a"].shape[1] // 2
    for name in ring_order(steps):
        step = int(name[2:])
        value = held[name[:2] + str(step - 1)]
        if step == steps:
            value = value[:, :middle] if name[0] == "r" else value[:, middle:]
        held[name] = lax.ppermute(value, "seq", right if name[0] == "r" else left)

    def put(mixed, *pieces):
        earlier = project(
            seq_count,
            [(offset, [held[f"{way}a{at}"]]) for offset, way, at in pieces],
            (0,),
            out_weight,
            finish=False,
        )
        return project(
            seq_count,
            [(offset, [held[f"{way}b{at}"]]) for offset, way, at in pieces],
            (0,),
            weight_other,
            earlier,
            mixed,
        )

    mixed = put(None, (0, "r", 0))
    for step in range(1, steps):
        mixed = put(mixed, (-step, "r", step), (step, "l", step))
    ends = (0, middle)
    pieces = [(steps, [held[f"ra{steps}"], held[f"la{steps}"]])]
    earlier = project(seq_count, pieces, ends, out_weight, finish=False)
    pieces = [(steps, [held[f"rb{steps}"], held[f"lb{steps}"]])]
    return project(seq_count, pieces, ends, weight_other, earlier, mixed)


def solution(mesh):
    placed = (
        P(("groups", "seq", "head"), None),
        P(("groups", "seq"), None),
        P(),
        P("head", None, None),
        P("head", None, None),
        P("head", "seq"),
    )
    return jax.shard_map(
        layer,
        mesh=mesh,
        in_specs=placed,
        out_specs=P("groups", "head", None, "seq"),
        check_vma=False,
    )
```

```python
import functools

import jax
import jax.numpy as jnp
import numpy as np
from jax import lax
from jax.experimental import pallas as pl
from jax.experimental.pallas import tpu as pltpu
from jax.sharding import PartitionSpec as P


KV = 512
ROPE = 64
NOPE = 128
VD = 128
QK = NOPE + ROPE
WIDE = KV + 2 * ROPE
EPS = 1e-06
HIDDEN = -1e30


def rope_angles(position, index):
    middle = ROPE // 2
    frequency = jnp.ones(index.shape, jnp.float32)
    for bit in range(middle.bit_length() - 1):
        factor = float(10000.0 ** (-(1 << bit) / middle))
        frequency *= jnp.where((index >> bit) % 2 == 1, factor, 1.0)
    return position.astype(jnp.float32) * frequency


def tag_lanes(rows, value):
    lane = lax.broadcasted_iota(jnp.int32, (rows, ROPE), 1)
    return value(lane).astype(jnp.bfloat16)


def prepare_kernel(half, latents, gain, full_out, half_out):
    block = lax.axis_index("seq")
    latent_f = latents[...].astype(jnp.float32)
    tokens = latent_f.shape[1]
    compressed = latent_f[:KV]
    spread = jnp.mean(compressed * compressed, axis=0, keepdims=True)
    normed = (compressed * lax.rsqrt(spread + EPS)).T * gain[...]
    full_out[:, :KV] = normed.astype(jnp.bfloat16)
    shape = (ROPE // 2, tokens)
    position = block * tokens + lax.broadcasted_iota(jnp.int32, shape, 1)
    angles = rope_angles(position, lax.broadcasted_iota(jnp.int32, shape, 0))
    cosine, sine = jnp.cos(angles), jnp.sin(angles)
    former, latter = latent_f[KV : KV + ROPE // 2], latent_f[KV + ROPE // 2 :]
    halves = [former * cosine - latter * sine, former * sine + latter * cosine]
    rope = jnp.concatenate(halves, 0).T.astype(jnp.bfloat16)
    tags = tag_lanes(tokens, lambda lane: jnp.where(lane == block, 1.0, 0.0))
    full_out[:, KV:] = jnp.concatenate([rope, tags], -1)
    start = lax.axis_index("head") * half
    half_out[...] = full_out[pl.ds(pl.multiple_of(start, half), half), :]


def prepare(latents, gain):
    rows = latents.shape[1]
    half = rows // 2
    return pl.pallas_call(
        functools.partial(prepare_kernel, half),
        out_shape=[
            jax.ShapeDtypeStruct((rows, WIDE), jnp.bfloat16),
            jax.ShapeDtypeStruct((half, WIDE), jnp.bfloat16),
        ],
        compiler_params=pltpu.CompilerParams(vmem_limit_bytes=12 << 20),
        cost_estimate=pl.CostEstimate(
            flops=10**8, bytes_accessed=4 * rows * WIDE, transcendentals=rows
        ),
        name="prepare",
    )(latents, gain)


def lift_kernel(queries, key_up, out):
    rows = queries.shape[0]
    heads = key_up.shape[0]
    block = lax.axis_index("seq")
    for head in range(heads):
        plain = queries[:, head * QK : head * QK + NOPE]
        lifted = jnp.dot(plain, key_up[head], preferred_element_type=jnp.float32)
        out[pl.ds(head * rows, rows), :KV] = lifted.astype(jnp.bfloat16)
    shape = (rows, ROPE)
    first = (2 * block + lax.axis_index("head")) * rows
    position = first + lax.broadcasted_iota(jnp.int32, shape, 0)
    lane = lax.broadcasted_iota(jnp.int32, shape, 1)
    upper = lane >= ROPE // 2
    angles = rope_angles(position, jnp.where(upper, lane - ROPE // 2, lane))
    cosine = jnp.concatenate([jnp.cos(angles)] * heads, 0)
    sine = jnp.sin(angles)
    sine = jnp.concatenate([jnp.where(upper, sine, -sine)] * heads, 0)
    turning = jnp.concatenate(
        [
            queries[:, head * QK + NOPE : (head + 1) * QK].astype(jnp.float32)
            for head in range(heads)
        ],
        0,
    )
    swapped = jnp.concatenate([turning[:, ROPE // 2 :], turning[:, : ROPE // 2]], -1)
    turned = (turning * cosine + swapped * sine).astype(jnp.bfloat16)
    tags = tag_lanes(heads * rows, lambda lane: jnp.where(lane > block, HIDDEN, 0.0))
    out[:, KV:] = jnp.concatenate([turned, tags], -1)


def lift(queries, key_up, other):
    rows = queries.shape[0]
    heads = key_up.shape[0]
    step = 8
    steps = heads // step

    def query_block(i):
        half = lax.axis_index("head")
        return (0, (1 - half if other else half) * steps + i)

    return pl.pallas_call(
        lift_kernel,
        grid=(steps,),
        in_specs=[
            pl.BlockSpec((rows, step * QK), query_block),
            pl.BlockSpec((step, NOPE, KV), lambda i: (i, 0, 0)),
        ],
        out_specs=pl.BlockSpec((step * rows, WIDE), lambda i: (i, 0)),
        out_shape=jax.ShapeDtypeStruct((heads * rows, WIDE), jnp.bfloat16),
        cost_estimate=pl.CostEstimate(
            flops=2 * heads * rows * NOPE * KV,
            bytes_accessed=2 * heads * (NOPE * KV + rows * (QK + WIDE)),
            transcendentals=0,
        ),
        compiler_params=pltpu.CompilerParams(vmem_limit_bytes=12 << 20),
        name="lift",
    )(queries, key_up)


def attend_kernel(part, groups, own, earlier, finish, query_rows, *refs):
    refs = list(refs)
    value_up = refs.pop(0) if finish else None
    old_sums, old_stats = (refs.pop(0), refs.pop(0)) if earlier else (None, None)
    groups, refs = refs[:groups], refs[groups:]
    keys = refs[-1]
    total = query_rows.shape[0]
    rows = total // 8

    @pl.when(pl.program_id(0) == 0)
    def _():
        start = 0
        for group in groups:
            keys[start : start + group.shape[0], :] = group[...]
            start += group.shape[0]

    factor = QK ** (-0.5) * float(np.log2(np.e))
    offset = lax.axis_index("head") * rows

    def score_rows(i):
        return lax.dot_general(
            query_rows[i * part : (i + 1) * part, :],
            keys[...],
            (((1,), (1,)), ((), ())),
            preferred_element_type=jnp.float32,
        )

    def complete(i, score):
        here = slice(i * part, (i + 1) * part)
        if own:
            query_pos = offset + lax.rem(lax.broadcasted_iota(jnp.int32, (part, own), 0), rows)
            key_pos = lax.broadcasted_iota(jnp.int32, (part, own), 1)
            diagonal = jnp.where(key_pos <= query_pos, score[:, :own], HIDDEN)
            score = jnp.concatenate([diagonal, score[:, own:]], 1)
        peak = jnp.max(score, axis=-1, keepdims=True)
        if earlier:
            old_peak = old_stats[here, :1]
            peak = jnp.maximum(peak, old_peak)
            carry = jnp.exp2((old_peak - peak) * factor)
        probs = jnp.exp2((score - peak) * factor)
        totals = jnp.sum(probs, axis=-1, keepdims=True)
        sums = jnp.dot(
            probs.astype(jnp.bfloat16), keys[:, :KV], preferred_element_type=jnp.float32
        )
        if earlier:
            totals += old_stats[here, 128:129] * carry
            sums += old_sums[here, :] * carry
        if not finish:
            refs[0][here, :] = sums
            refs[1][here, :128] = jnp.broadcast_to(peak, (part, 128))
            refs[1][here, 128:] = jnp.broadcast_to(totals, (part, 128))
            return
        latent_out = (sums / totals).astype(jnp.bfloat16)
        for j in range(part // rows):
            head = i * (part // rows) + j
            piece = jnp.dot(
                latent_out[j * rows : (j + 1) * rows],
                value_up[head],
                preferred_element_type=jnp.float32,
            )
            refs[0][:, head * VD : (head + 1) * VD] = piece.astype(jnp.bfloat16)

    count = total // part
    score = score_rows(0)
    for i in range(count):
        later = score_rows(i + 1) if i + 1 < count else None
        complete(i, score)
        score = later


def attend(query_rows, keys, rows, blocks, own=0, value_up=None, earlier=()):
    step = 8
    first, count = blocks
    heads = count * step
    key_total = sum(key.shape[0] for key in keys)
    finish = value_up is not None
    operands, specs = [query_rows], [pl.BlockSpec((step * rows, WIDE), lambda i: (first + i, 0))]
    if finish:
        operands.append(value_up)
        specs.append(pl.BlockSpec((step, KV, VD), lambda i: (first + i, 0, 0)))
    for value in earlier:
        operands.append(value)
        specs.append(pl.BlockSpec((step * rows, value.shape[1]), lambda i: (i, 0)))
    operands += keys
    specs += [pl.BlockSpec(key.shape, lambda i: (0, 0)) for key in keys]
    if finish:
        outs = jax.ShapeDtypeStruct((rows, heads * VD), jnp.bfloat16)
        out_specs = pl.BlockSpec((rows, step * VD), lambda i: (0, i))
    else:
        outs = [jax.ShapeDtypeStruct((heads * rows, width), jnp.float32) for width in (KV, 256)]
        out_specs = [
            pl.BlockSpec((step * rows, width), lambda i: (i, 0)) for width in (KV, 256)
        ]
    return pl.pallas_call(
        functools.partial(
            attend_kernel, 4 * rows, len(keys), own, bool(earlier), finish
        ),
        grid=(count,),
        in_specs=specs,
        out_specs=out_specs,
        out_shape=outs,
        scratch_shapes=[pltpu.VMEM((key_total, WIDE), jnp.bfloat16)],
        cost_estimate=pl.CostEstimate(
            flops=2 * heads * rows * (key_total * (WIDE + KV) + KV * VD),
            bytes_accessed=2 * heads * (KV * VD + rows * (WIDE + VD)) + 2 * key_total * WIDE,
            transcendentals=heads * rows * key_total,
        ),
        compiler_params=pltpu.CompilerParams(
            vmem_limit_bytes=(16 << 20) + 16 * key_total * WIDE
        ),
        name="attend",
    )(*operands)


def project_kernel(count, offsets, rows_of, finish, added, *refs):
    pieces, chunks = len(offsets), len(rows_of)
    parts = refs[: pieces * chunks]
    weight = refs[pieces * chunks]
    product = None
    for chunk, start in enumerate(rows_of):
        stack = [parts[piece * chunks + chunk][...] for piece in range(pieces)]
        stack = jnp.concatenate(stack, 0) if pieces > 1 else stack[0]
        part = jnp.dot(
            stack,
            weight[start : start + stack.shape[1], :],
            preferred_element_type=jnp.float32,
        )
        product = part if product is None else product + part
    if added:
        product += refs[pieces * chunks + 1][...]
    if not finish:
        refs[-1][...] = product
        return
    out, held, sems = refs[-3:]
    rows = parts[0].shape[0]
    held[...] = product.astype(jnp.bfloat16)
    block = lax.axis_index("seq")
    half = block // 2
    place = jnp.where(block - 2 * half == 0, half, count - 1 - half)
    copies = []
    for i, offset in enumerate(offsets):
        at = lax.rem(place + offset % count, count)
        source = jnp.where(at < count // 2, 2 * at, 2 * (count - 1 - at) + 1)
        copies.append(
            pltpu.make_async_copy(held.at[pl.ds(i * rows, rows), :], out.at[source, 0], sems.at[i])
        )
        copies[-1].start()
    for copy in copies:
        copy.wait()


def project(count, pieces, rows_of, weight, earlier=None, mixed=None, finish=True):
    offsets = [offset for offset, _ in pieces]
    operands = [part for _, parts in pieces for part in parts]
    rows = operands[0].shape[0]
    columns = weight.shape[1]
    total = len(pieces) * rows
    operands.append(weight)
    if earlier is not None:
        operands.append(earlier)
    aliases = {}
    vmem = pl.BlockSpec(memory_space=pltpu.VMEM)
    anywhere = pl.BlockSpec(memory_space=pl.ANY)
    specs = [vmem] * len(operands)
    if finish and mixed is not None:
        aliases = {len(operands): 0}
        operands.append(mixed)
        specs.append(anywhere)
    if finish:
        shape = jax.ShapeDtypeStruct((count, 1, rows, columns), jnp.bfloat16)
        scratch = [
            pltpu.VMEM((total, columns), jnp.bfloat16),
            pltpu.SemaphoreType.DMA((len(pieces),)),
        ]
    else:
        shape = jax.ShapeDtypeStruct((total, columns), jnp.float32)
        scratch = []
    return pl.pallas_call(
        functools.partial(
            project_kernel, count, offsets, rows_of, finish, earlier is not None
        ),
        in_specs=specs,
        out_specs=anywhere if finish else vmem,
        out_shape=shape,
        scratch_shapes=scratch,
        input_output_aliases=aliases,
        compiler_params=pltpu.CompilerParams(vmem_limit_bytes=8 << 20),
        cost_estimate=pl.CostEstimate(
            flops=2 * total * weight.shape[0] * columns,
            bytes_accessed=2 * weight.shape[0] * columns,
            transcendentals=0,
        ),
        name="project",
    )(*operands)


def gather_plan(count):
    moves = []
    bit = count // 2
    slots = [0]
    while bit:
        moves += [(slot, bit) for slot in slots]
        slots += [slot | bit for slot in slots]
        bit //= 2
    return moves


def ring_order(steps):
    names = ["ra1", "la1", "rx1", "lx1", "ry1", "ly1"]
    names += ["ra2", "la2", "rb2", "lb2"]
    return names + [
        way + chunk + str(step) for step in range(3, steps + 1) for chunk in "ab" for way in "rl"
    ]


def layer(queries, latents, latent_gain, key_up, value_up, out_weight):
    seq_count = lax.axis_size("seq")
    head_count = lax.axis_size("head")
    rows = queries.shape[0]
    swap_pairs = [(i, (i + 1) % head_count) for i in range(head_count)]
    everyone = range(seq_count)

    own_keys, half_keys = prepare(latents.T, latent_gain.reshape(1, KV))
    slots = {0: half_keys}
    for slot, bit in gather_plan(seq_count):
        slots[slot | bit] = lax.ppermute(slots[slot], "seq", [(d ^ bit, d) for d in everyone])
    near = [m for m in range(1, seq_count) if m % 2 == 0] + [1]
    far = [m for m in range(2, seq_count) if m % 2 == 1]
    near_keys = jnp.concatenate([slots[m] for m in near], 0)
    far_keys = jnp.concatenate([slots[m] for m in far], 0)
    near_swap = lax.ppermute(near_keys, "head", swap_pairs)
    far_swap = lax.ppermute(far_keys, "head", swap_pairs)

    key_other = lax.ppermute(key_up, "head", swap_pairs)
    value_other = lax.ppermute(value_up, "head", swap_pairs)
    weight_other = lax.ppermute(out_weight, "head", swap_pairs)
    rows_a = lift(queries, key_up, False)
    rows_b = lift(queries, key_other, True)
    count = key_up.shape[0] // 8
    early = [own_keys, near_keys, near_swap] + [slots[m] for m in far[:-1]]
    late = [slots[far[-1]], far_swap]
    keys = [own_keys, near_keys, near_swap, far_keys, far_swap]
    own = own_keys.shape[0]
    running = attend(rows_a, early, rows, (0, count), own)
    heads_a = attend(rows_a, late, rows, (0, count), 0, value_up, running)
    heads_x = attend(rows_b, keys, rows, (0, count // 2), own, value_other)
    heads_y = attend(rows_b, keys, rows, (count // 2, count - count // 2), own, value_other)

    order = list(range(0, seq_count, 2)) + list(range(seq_count - 1, 0, -2))
    right = [(order[i], order[(i + 1) % seq_count]) for i in everyone]
    left = [(b, a) for a, b in right]
    steps = seq_count // 2
    held = {way + "a0": heads_a for way in "rl"}
    for way in "rl":
        held[way + "x0"], held[way + "y0"] = heads_x, heads_y
    middle = heads_a.shape[1] // 2
    for name in ring_order(steps):
        step = int(name[2:])
        value = held[name[:2] + str(step - 1)]
        if step == steps:
            value = value[:, :middle] if name[0] == "r" else value[:, middle:]
        held[name] = lax.ppermute(value, "seq", right if name[0] == "r" else left)
        if name[1:] == "y1":
            parts = [held[name[0] + "x1"], held[name]]
            held[name[0] + "b1"] = jnp.concatenate(parts, 1)

    def put(mixed, *pieces):
        earlier = project(
            seq_count,
            [(offset, [held[f"{way}a{at}"]]) for offset, way, at in pieces],
            (0,),
            out_weight,
            finish=False,
        )
        return project(
            seq_count,
            [(offset, [held[f"{way}b{at}"]]) for offset, way, at in pieces],
            (0,),
            weight_other,
            earlier,
            mixed,
        )

    earlier = project(seq_count, [(0, [heads_a])], (0,), out_weight, finish=False)
    pieces = [(0, [heads_x, heads_y])]
    mixed = project(seq_count, pieces, (0, middle), weight_other, earlier)
    for step in range(1, steps):
        mixed = put(mixed, (-step, "r", step), (step, "l", step))
    ends = (0, middle)
    pieces = [(steps, [held[f"ra{steps}"], held[f"la{steps}"]])]
    earlier = project(seq_count, pieces, ends, out_weight, finish=False)
    pieces = [(steps, [held[f"rb{steps}"], held[f"lb{steps}"]])]
    return project(seq_count, pieces, ends, weight_other, earlier, mixed)


def solution(mesh):
    placed = (
        P(("groups", "seq", "head"), None),
        P(("groups", "seq"), None),
        P(),
        P("head", None, None),
        P("head", None, None),
        P("head", "seq"),
    )
    return jax.shard_map(
        layer,
        mesh=mesh,
        in_specs=placed,
        out_specs=P("groups", "head", None, "seq"),
        check_vma=False,
    )
```

```python
import functools

import jax
import jax.numpy as jnp
import numpy as np
from jax import lax
from jax.experimental import pallas as pl
from jax.experimental.pallas import tpu as pltpu
from jax.sharding import PartitionSpec as P


KV = 512
ROPE = 64
NOPE = 128
VD = 128
QK = NOPE + ROPE
WIDE = KV + 2 * ROPE
EPS = 1e-06
HIDDEN = -1e30


def rope_angles(position, index):
    middle = ROPE // 2
    frequency = jnp.ones(index.shape, jnp.float32)
    for bit in range(middle.bit_length() - 1):
        factor = float(10000.0 ** (-(1 << bit) / middle))
        frequency *= jnp.where((index >> bit) % 2 == 1, factor, 1.0)
    return position.astype(jnp.float32) * frequency


def tag_lanes(rows, value):
    lane = lax.broadcasted_iota(jnp.int32, (rows, ROPE), 1)
    return value(lane).astype(jnp.bfloat16)


def prepare_kernel(half, latents, gain, full_out, half_out):
    block = lax.axis_index("seq")
    latent_f = latents[...].astype(jnp.float32)
    tokens = latent_f.shape[1]
    compressed = latent_f[:KV]
    spread = jnp.mean(compressed * compressed, axis=0, keepdims=True)
    normed = (compressed * lax.rsqrt(spread + EPS)).T * gain[...]
    full_out[:, :KV] = normed.astype(jnp.bfloat16)
    shape = (ROPE // 2, tokens)
    position = block * tokens + lax.broadcasted_iota(jnp.int32, shape, 1)
    angles = rope_angles(position, lax.broadcasted_iota(jnp.int32, shape, 0))
    cosine, sine = jnp.cos(angles), jnp.sin(angles)
    former, latter = latent_f[KV : KV + ROPE // 2], latent_f[KV + ROPE // 2 :]
    halves = [former * cosine - latter * sine, former * sine + latter * cosine]
    rope = jnp.concatenate(halves, 0).T.astype(jnp.bfloat16)
    tags = tag_lanes(tokens, lambda lane: jnp.where(lane == block, 1.0, 0.0))
    full_out[:, KV:] = jnp.concatenate([rope, tags], -1)
    start = lax.axis_index("head") * half
    half_out[...] = full_out[pl.ds(pl.multiple_of(start, half), half), :]


def prepare(latents, gain):
    rows = latents.shape[1]
    half = rows // 2
    return pl.pallas_call(
        functools.partial(prepare_kernel, half),
        out_shape=[
            jax.ShapeDtypeStruct((rows, WIDE), jnp.bfloat16),
            jax.ShapeDtypeStruct((half, WIDE), jnp.bfloat16),
        ],
        compiler_params=pltpu.CompilerParams(vmem_limit_bytes=12 << 20),
        cost_estimate=pl.CostEstimate(
            flops=10**8, bytes_accessed=4 * rows * WIDE, transcendentals=rows
        ),
        name="prepare",
    )(latents, gain)


def lift_kernel(queries, key_up, out):
    rows = queries.shape[0]
    heads = key_up.shape[0]
    block = lax.axis_index("seq")
    for head in range(heads):
        plain = queries[:, head * QK : head * QK + NOPE]
        lifted = jnp.dot(plain, key_up[head], preferred_element_type=jnp.float32)
        out[pl.ds(head * rows, rows), :KV] = lifted.astype(jnp.bfloat16)
    shape = (rows, ROPE)
    first = (2 * block + lax.axis_index("head")) * rows
    position = first + lax.broadcasted_iota(jnp.int32, shape, 0)
    lane = lax.broadcasted_iota(jnp.int32, shape, 1)
    upper = lane >= ROPE // 2
    angles = rope_angles(position, jnp.where(upper, lane - ROPE // 2, lane))
    cosine = jnp.concatenate([jnp.cos(angles)] * heads, 0)
    sine = jnp.sin(angles)
    sine = jnp.concatenate([jnp.where(upper, sine, -sine)] * heads, 0)
    turning = jnp.concatenate(
        [
            queries[:, head * QK + NOPE : (head + 1) * QK].astype(jnp.float32)
            for head in range(heads)
        ],
        0,
    )
    swapped = jnp.concatenate([turning[:, ROPE // 2 :], turning[:, : ROPE // 2]], -1)
    turned = (turning * cosine + swapped * sine).astype(jnp.bfloat16)
    tags = tag_lanes(heads * rows, lambda lane: jnp.where(lane > block, HIDDEN, 0.0))
    out[:, KV:] = jnp.concatenate([turned, tags], -1)


def lift(queries, key_up, other):
    rows = queries.shape[0]
    heads = key_up.shape[0]
    step = 8
    steps = heads // step

    def query_block(i):
        half = lax.axis_index("head")
        return (0, (1 - half if other else half) * steps + i)

    return pl.pallas_call(
        lift_kernel,
        grid=(steps,),
        in_specs=[
            pl.BlockSpec((rows, step * QK), query_block),
            pl.BlockSpec((step, NOPE, KV), lambda i: (i, 0, 0)),
        ],
        out_specs=pl.BlockSpec((step * rows, WIDE), lambda i: (i, 0)),
        out_shape=jax.ShapeDtypeStruct((heads * rows, WIDE), jnp.bfloat16),
        cost_estimate=pl.CostEstimate(
            flops=2 * heads * rows * NOPE * KV,
            bytes_accessed=2 * heads * (NOPE * KV + rows * (QK + WIDE)),
            transcendentals=0,
        ),
        compiler_params=pltpu.CompilerParams(vmem_limit_bytes=12 << 20),
        name="lift",
    )(queries, key_up)


def attend_kernel(offset_rows, part, groups, own, earlier, finish, query_rows, *refs):
    refs = list(refs)
    value_up = refs.pop(0) if finish else None
    old_sums, old_stats = (refs.pop(0), refs.pop(0)) if earlier else (None, None)
    groups, refs = refs[:groups], refs[groups:]
    keys = refs[-1]
    total = query_rows.shape[0]
    rows = offset_rows

    @pl.when(pl.program_id(0) == 0)
    def _():
        start = 0
        for group in groups:
            keys[start : start + group.shape[0], :] = group[...]
            start += group.shape[0]

    factor = QK ** (-0.5) * float(np.log2(np.e))
    offset = lax.axis_index("head") * rows

    def score_rows(i):
        return lax.dot_general(
            query_rows[i * part : (i + 1) * part, :],
            keys[...],
            (((1,), (1,)), ((), ())),
            preferred_element_type=jnp.float32,
        )

    def complete(i, score):
        here = slice(i * part, (i + 1) * part)
        if own:
            query_pos = offset + lax.rem(lax.broadcasted_iota(jnp.int32, (part, own), 0), rows)
            key_pos = lax.broadcasted_iota(jnp.int32, (part, own), 1)
            diagonal = jnp.where(key_pos <= query_pos, score[:, :own], HIDDEN)
            score = jnp.concatenate([diagonal, score[:, own:]], 1)
        peak = jnp.max(score, axis=-1, keepdims=True)
        if earlier:
            old_peak = old_stats[here, :1]
            peak = jnp.maximum(peak, old_peak)
            carry = jnp.exp2((old_peak - peak) * factor)
        probs = jnp.exp2((score - peak) * factor)
        totals = jnp.sum(probs, axis=-1, keepdims=True)
        sums = jnp.dot(
            probs.astype(jnp.bfloat16), keys[:, :KV], preferred_element_type=jnp.float32
        )
        if earlier:
            totals += old_stats[here, 128:129] * carry
            sums += old_sums[here, :] * carry
        if not finish:
            refs[0][here, :] = sums
            refs[1][here, :128] = jnp.broadcast_to(peak, (part, 128))
            refs[1][here, 128:] = jnp.broadcast_to(totals, (part, 128))
            return
        latent_out = (sums / totals).astype(jnp.bfloat16)
        for j in range(part // rows):
            head = i * (part // rows) + j
            piece = jnp.dot(
                latent_out[j * rows : (j + 1) * rows],
                value_up[head],
                preferred_element_type=jnp.float32,
            )
            refs[0][:, head * VD : (head + 1) * VD] = piece.astype(jnp.bfloat16)

    count = total // part
    score = score_rows(0)
    for i in range(count):
        later = score_rows(i + 1) if i + 1 < count else None
        complete(i, score)
        score = later


def attend(query_rows, keys, rows, blocks, own=0, value_up=None, earlier=()):
    step = 8
    first, count = blocks
    heads = count * step
    if first == 0:
        step, count = heads, 1
    key_total = sum(key.shape[0] for key in keys)
    finish = value_up is not None
    operands, specs = [query_rows], [pl.BlockSpec((step * rows, WIDE), lambda i: (first + i, 0))]
    if finish:
        operands.append(value_up)
        specs.append(pl.BlockSpec((step, KV, VD), lambda i: (first + i, 0, 0)))
    for value in earlier:
        operands.append(value)
        specs.append(pl.BlockSpec((step * rows, value.shape[1]), lambda i: (i, 0)))
    operands += keys
    specs += [pl.BlockSpec(key.shape, lambda i: (0, 0)) for key in keys]
    if finish:
        outs = jax.ShapeDtypeStruct((rows, heads * VD), jnp.bfloat16)
        out_specs = pl.BlockSpec((rows, step * VD), lambda i: (0, i))
    else:
        outs = [jax.ShapeDtypeStruct((heads * rows, width), jnp.float32) for width in (KV, 256)]
        out_specs = [
            pl.BlockSpec((step * rows, width), lambda i: (i, 0)) for width in (KV, 256)
        ]
    return pl.pallas_call(
        functools.partial(
            attend_kernel, rows, 4 * rows, len(keys), own, bool(earlier), finish
        ),
        grid=(count,),
        in_specs=specs,
        out_specs=out_specs,
        out_shape=outs,
        scratch_shapes=[pltpu.VMEM((key_total, WIDE), jnp.bfloat16)],
        cost_estimate=pl.CostEstimate(
            flops=2 * heads * rows * (key_total * (WIDE + KV) + KV * VD),
            bytes_accessed=2 * heads * (KV * VD + rows * (WIDE + VD)) + 2 * key_total * WIDE,
            transcendentals=heads * rows * key_total,
        ),
        compiler_params=pltpu.CompilerParams(
            vmem_limit_bytes=(16 << 20) + 16 * key_total * WIDE
        ),
        name="attend",
    )(*operands)


def project_kernel(count, offsets, rows_of, finish, added, *refs):
    pieces, chunks = len(offsets), len(rows_of)
    parts = refs[: pieces * chunks]
    weight = refs[pieces * chunks]
    product = None
    for chunk, start in enumerate(rows_of):
        stack = [parts[piece * chunks + chunk][...] for piece in range(pieces)]
        stack = jnp.concatenate(stack, 0) if pieces > 1 else stack[0]
        part = jnp.dot(
            stack,
            weight[start : start + stack.shape[1], :],
            preferred_element_type=jnp.float32,
        )
        product = part if product is None else product + part
    if added:
        product += refs[pieces * chunks + 1][...]
    if not finish:
        refs[-1][...] = product
        return
    out, held, sems = refs[-3:]
    rows = parts[0].shape[0]
    held[...] = product.astype(jnp.bfloat16)
    block = lax.axis_index("seq")
    half = block // 2
    place = jnp.where(block - 2 * half == 0, half, count - 1 - half)
    copies = []
    for i, offset in enumerate(offsets):
        at = lax.rem(place + offset % count, count)
        source = jnp.where(at < count // 2, 2 * at, 2 * (count - 1 - at) + 1)
        copies.append(
            pltpu.make_async_copy(held.at[pl.ds(i * rows, rows), :], out.at[source, 0], sems.at[i])
        )
        copies[-1].start()
    for copy in copies:
        copy.wait()


def project(count, pieces, rows_of, weight, earlier=None, mixed=None, finish=True):
    offsets = [offset for offset, _ in pieces]
    operands = [part for _, parts in pieces for part in parts]
    rows = operands[0].shape[0]
    columns = weight.shape[1]
    total = len(pieces) * rows
    operands.append(weight)
    if earlier is not None:
        operands.append(earlier)
    aliases = {}
    vmem = pl.BlockSpec(memory_space=pltpu.VMEM)
    anywhere = pl.BlockSpec(memory_space=pl.ANY)
    specs = [vmem] * len(operands)
    if finish and mixed is not None:
        aliases = {len(operands): 0}
        operands.append(mixed)
        specs.append(anywhere)
    if finish:
        shape = jax.ShapeDtypeStruct((count, 1, rows, columns), jnp.bfloat16)
        scratch = [
            pltpu.VMEM((total, columns), jnp.bfloat16),
            pltpu.SemaphoreType.DMA((len(pieces),)),
        ]
    else:
        shape = jax.ShapeDtypeStruct((total, columns), jnp.float32)
        scratch = []
    return pl.pallas_call(
        functools.partial(
            project_kernel, count, offsets, rows_of, finish, earlier is not None
        ),
        in_specs=specs,
        out_specs=anywhere if finish else vmem,
        out_shape=shape,
        scratch_shapes=scratch,
        input_output_aliases=aliases,
        compiler_params=pltpu.CompilerParams(vmem_limit_bytes=8 << 20),
        cost_estimate=pl.CostEstimate(
            flops=2 * total * weight.shape[0] * columns,
            bytes_accessed=2 * weight.shape[0] * columns,
            transcendentals=0,
        ),
        name="project",
    )(*operands)


def gather_plan(count):
    moves = []
    bit = count // 2
    slots = [0]
    while bit:
        moves += [(slot, bit) for slot in slots]
        slots += [slot | bit for slot in slots]
        bit //= 2
    return moves


def ring_order(steps):
    names = ["ra1", "la1", "rx1", "lx1", "ry1", "ly1"]
    names += ["ra2", "la2", "rb2", "lb2"]
    return names + [
        way + chunk + str(step) for step in range(3, steps + 1) for chunk in "ab" for way in "rl"
    ]


def layer(queries, latents, latent_gain, key_up, value_up, out_weight):
    seq_count = lax.axis_size("seq")
    head_count = lax.axis_size("head")
    rows = queries.shape[0]
    swap_pairs = [(i, (i + 1) % head_count) for i in range(head_count)]
    everyone = range(seq_count)

    own_keys, half_keys = prepare(latents.T, latent_gain.reshape(1, KV))
    slots = {0: half_keys}
    for slot, bit in gather_plan(seq_count):
        slots[slot | bit] = lax.ppermute(slots[slot], "seq", [(d ^ bit, d) for d in everyone])
    near = [m for m in range(1, seq_count) if m % 2 == 0] + [1]
    far = [m for m in range(2, seq_count) if m % 2 == 1]
    near_keys = jnp.concatenate([slots[m] for m in near], 0)
    far_keys = jnp.concatenate([slots[m] for m in far], 0)
    near_swap = lax.ppermute(near_keys, "head", swap_pairs)
    far_swap = lax.ppermute(far_keys, "head", swap_pairs)

    key_other = lax.ppermute(key_up, "head", swap_pairs)
    value_other = lax.ppermute(value_up, "head", swap_pairs)
    weight_other = lax.ppermute(out_weight, "head", swap_pairs)
    rows_a = lift(queries, key_up, False)
    rows_b = lift(queries, key_other, True)
    count = key_up.shape[0] // 8
    early = [own_keys, near_keys, near_swap] + [slots[m] for m in far[:-1]]
    late = [slots[far[-1]], far_swap]
    keys = [own_keys, near_keys, near_swap, far_keys, far_swap]
    own = own_keys.shape[0]
    running = attend(rows_a, early, rows, (0, count), own)
    heads_a = attend(rows_a, late, rows, (0, count), 0, value_up, running)
    heads_x = attend(rows_b, keys, rows, (0, count // 2), own, value_other)
    heads_y = attend(rows_b, keys, rows, (count // 2, count - count // 2), own, value_other)

    order = list(range(0, seq_count, 2)) + list(range(seq_count - 1, 0, -2))
    right = [(order[i], order[(i + 1) % seq_count]) for i in everyone]
    left = [(b, a) for a, b in right]
    steps = seq_count // 2
    held = {way + "a0": heads_a for way in "rl"}
    for way in "rl":
        held[way + "x0"], held[way + "y0"] = heads_x, heads_y
    middle = heads_a.shape[1] // 2
    for name in ring_order(steps):
        step = int(name[2:])
        value = held[name[:2] + str(step - 1)]
        if step == steps:
            value = value[:, :middle] if name[0] == "r" else value[:, middle:]
        held[name] = lax.ppermute(value, "seq", right if name[0] == "r" else left)
        if name[1:] == "y1":
            parts = [held[name[0] + "x1"], held[name]]
            held[name[0] + "b1"] = jnp.concatenate(parts, 1)

    def put(mixed, *pieces):
        earlier = project(
            seq_count,
            [(offset, [held[f"{way}a{at}"]]) for offset, way, at in pieces],
            (0,),
            out_weight,
            finish=False,
        )
        return project(
            seq_count,
            [(offset, [held[f"{way}b{at}"]]) for offset, way, at in pieces],
            (0,),
            weight_other,
            earlier,
            mixed,
        )

    earlier = project(seq_count, [(0, [heads_a])], (0,), out_weight, finish=False)
    pieces = [(0, [heads_x, heads_y])]
    mixed = project(seq_count, pieces, (0, middle), weight_other, earlier)
    for step in range(1, steps):
        mixed = put(mixed, (-step, "r", step), (step, "l", step))
    ends = (0, middle)
    pieces = [(steps, [held[f"ra{steps}"], held[f"la{steps}"]])]
    earlier = project(seq_count, pieces, ends, out_weight, finish=False)
    pieces = [(steps, [held[f"rb{steps}"], held[f"lb{steps}"]])]
    return project(seq_count, pieces, ends, weight_other, earlier, mixed)


def solution(mesh):
    placed = (
        P(("groups", "seq", "head"), None),
        P(("groups", "seq"), None),
        P(),
        P("head", None, None),
        P("head", None, None),
        P("head", "seq"),
    )
    return jax.shard_map(
        layer,
        mesh=mesh,
        in_specs=placed,
        out_specs=P("groups", "head", None, "seq"),
        check_vma=False,
    )
```

```python
import functools

import jax
import jax.numpy as jnp
import numpy as np
from jax import lax
from jax.experimental import pallas as pl
from jax.experimental.pallas import tpu as pltpu
from jax.sharding import PartitionSpec as P


KV = 512
ROPE = 64
NOPE = 128
VD = 128
QK = NOPE + ROPE
WIDE = KV + 2 * ROPE
EPS = 1e-06
HIDDEN = -1e30


def rope_angles(position, index):
    middle = ROPE // 2
    frequency = jnp.ones(index.shape, jnp.float32)
    for bit in range(middle.bit_length() - 1):
        factor = float(10000.0 ** (-(1 << bit) / middle))
        frequency *= jnp.where((index >> bit) % 2 == 1, factor, 1.0)
    return position.astype(jnp.float32) * frequency


def tag_lanes(rows, value):
    lane = lax.broadcasted_iota(jnp.int32, (rows, ROPE), 1)
    return value(lane).astype(jnp.bfloat16)


def prepare_kernel(half, latents, gain, full_out, half_out):
    block = lax.axis_index("seq")
    latent_f = latents[...].astype(jnp.float32)
    tokens = latent_f.shape[1]
    compressed = latent_f[:KV]
    spread = jnp.mean(compressed * compressed, axis=0, keepdims=True)
    normed = (compressed * lax.rsqrt(spread + EPS)).T * gain[...]
    full_out[:, :KV] = normed.astype(jnp.bfloat16)
    shape = (ROPE // 2, tokens)
    position = block * tokens + lax.broadcasted_iota(jnp.int32, shape, 1)
    angles = rope_angles(position, lax.broadcasted_iota(jnp.int32, shape, 0))
    cosine, sine = jnp.cos(angles), jnp.sin(angles)
    former, latter = latent_f[KV : KV + ROPE // 2], latent_f[KV + ROPE // 2 :]
    halves = [former * cosine - latter * sine, former * sine + latter * cosine]
    rope = jnp.concatenate(halves, 0).T.astype(jnp.bfloat16)
    tags = tag_lanes(tokens, lambda lane: jnp.where(lane == block, 1.0, 0.0))
    full_out[:, KV:] = jnp.concatenate([rope, tags], -1)
    start = lax.axis_index("head") * half
    half_out[...] = full_out[pl.ds(pl.multiple_of(start, half), half), :]


def prepare(latents, gain):
    rows = latents.shape[1]
    half = rows // 2
    return pl.pallas_call(
        functools.partial(prepare_kernel, half),
        out_shape=[
            jax.ShapeDtypeStruct((rows, WIDE), jnp.bfloat16),
            jax.ShapeDtypeStruct((half, WIDE), jnp.bfloat16),
        ],
        compiler_params=pltpu.CompilerParams(vmem_limit_bytes=12 << 20),
        cost_estimate=pl.CostEstimate(
            flops=10**8, bytes_accessed=4 * rows * WIDE, transcendentals=rows
        ),
        name="prepare",
    )(latents, gain)


def lift_kernel(queries, key_up, out):
    rows = queries.shape[0]
    heads = key_up.shape[0]
    block = lax.axis_index("seq")
    for head in range(heads):
        plain = queries[:, head * QK : head * QK + NOPE]
        lifted = jnp.dot(plain, key_up[head], preferred_element_type=jnp.float32)
        out[pl.ds(head * rows, rows), :KV] = lifted.astype(jnp.bfloat16)
    shape = (rows, ROPE)
    first = (2 * block + lax.axis_index("head")) * rows
    position = first + lax.broadcasted_iota(jnp.int32, shape, 0)
    lane = lax.broadcasted_iota(jnp.int32, shape, 1)
    upper = lane >= ROPE // 2
    angles = rope_angles(position, jnp.where(upper, lane - ROPE // 2, lane))
    cosine = jnp.concatenate([jnp.cos(angles)] * heads, 0)
    sine = jnp.sin(angles)
    sine = jnp.concatenate([jnp.where(upper, sine, -sine)] * heads, 0)
    turning = jnp.concatenate(
        [
            queries[:, head * QK + NOPE : (head + 1) * QK].astype(jnp.float32)
            for head in range(heads)
        ],
        0,
    )
    swapped = jnp.concatenate([turning[:, ROPE // 2 :], turning[:, : ROPE // 2]], -1)
    turned = (turning * cosine + swapped * sine).astype(jnp.bfloat16)
    tags = tag_lanes(heads * rows, lambda lane: jnp.where(lane > block, HIDDEN, 0.0))
    out[:, KV:] = jnp.concatenate([turned, tags], -1)


def lift(queries, key_up, other):
    rows = queries.shape[0]
    heads = key_up.shape[0]
    step = 8
    steps = heads // step

    def query_block(i):
        half = lax.axis_index("head")
        return (0, (1 - half if other else half) * steps + i)

    return pl.pallas_call(
        lift_kernel,
        grid=(steps,),
        in_specs=[
            pl.BlockSpec((rows, step * QK), query_block),
            pl.BlockSpec((step, NOPE, KV), lambda i: (i, 0, 0)),
        ],
        out_specs=pl.BlockSpec((step * rows, WIDE), lambda i: (i, 0)),
        out_shape=jax.ShapeDtypeStruct((heads * rows, WIDE), jnp.bfloat16),
        cost_estimate=pl.CostEstimate(
            flops=2 * heads * rows * NOPE * KV,
            bytes_accessed=2 * heads * (NOPE * KV + rows * (QK + WIDE)),
            transcendentals=0,
        ),
        compiler_params=pltpu.CompilerParams(vmem_limit_bytes=12 << 20),
        name="lift",
    )(queries, key_up)


def attend_kernel(offset_rows, part, groups, own, earlier, finish, query_rows, *refs):
    refs = list(refs)
    value_up = refs.pop(0) if finish else None
    old_sums, old_stats = (refs.pop(0), refs.pop(0)) if earlier else (None, None)
    groups, refs = refs[:groups], refs[groups:]
    keys = refs[-1]
    total = query_rows.shape[0]
    rows = offset_rows

    @pl.when(pl.program_id(0) == 0)
    def _():
        start = 0
        for group in groups:
            keys[start : start + group.shape[0], :] = group[...]
            start += group.shape[0]

    factor = QK ** (-0.5) * float(np.log2(np.e))
    offset = lax.axis_index("head") * rows

    def score_rows(i):
        return lax.dot_general(
            query_rows[i * part : (i + 1) * part, :],
            keys[...],
            (((1,), (1,)), ((), ())),
            preferred_element_type=jnp.float32,
        )

    def complete(i, score):
        here = slice(i * part, (i + 1) * part)
        if own:
            query_pos = offset + lax.rem(lax.broadcasted_iota(jnp.int32, (part, own), 0), rows)
            key_pos = lax.broadcasted_iota(jnp.int32, (part, own), 1)
            diagonal = jnp.where(key_pos <= query_pos, score[:, :own], HIDDEN)
            score = jnp.concatenate([diagonal, score[:, own:]], 1)
        peak = jnp.max(score, axis=-1, keepdims=True)
        if earlier:
            old_peak = old_stats[here, :1]
            peak = jnp.maximum(peak, old_peak)
            carry = jnp.exp2((old_peak - peak) * factor)
        probs = jnp.exp2((score - peak) * factor)
        totals = jnp.sum(probs, axis=-1, keepdims=True)
        sums = jnp.dot(
            probs.astype(jnp.bfloat16), keys[:, :KV], preferred_element_type=jnp.float32
        )
        if earlier:
            totals += old_stats[here, 128:129] * carry
            sums += old_sums[here, :] * carry
        if not finish:
            refs[0][here, :] = sums
            refs[1][here, :128] = jnp.broadcast_to(peak, (part, 128))
            refs[1][here, 128:] = jnp.broadcast_to(totals, (part, 128))
            return
        latent_out = (sums / totals).astype(jnp.bfloat16)
        for j in range(part // rows):
            head = i * (part // rows) + j
            piece = jnp.dot(
                latent_out[j * rows : (j + 1) * rows],
                value_up[head],
                preferred_element_type=jnp.float32,
            )
            refs[0][:, head * VD : (head + 1) * VD] = piece.astype(jnp.bfloat16)

    count = total // part
    score = score_rows(0)
    for i in range(count):
        later = score_rows(i + 1) if i + 1 < count else None
        complete(i, score)
        score = later


def attend(query_rows, keys, rows, blocks, own=0, value_up=None, earlier=()):
    step = 8
    first, count = blocks
    heads = count * step
    if first == 0:
        step, count = heads, 1
    key_total = sum(key.shape[0] for key in keys)
    finish = value_up is not None
    operands, specs = [query_rows], [pl.BlockSpec((step * rows, WIDE), lambda i: (first + i, 0))]
    if finish:
        operands.append(value_up)
        specs.append(pl.BlockSpec((step, KV, VD), lambda i: (first + i, 0, 0)))
    for value in earlier:
        operands.append(value)
        specs.append(pl.BlockSpec((step * rows, value.shape[1]), lambda i: (i, 0)))
    operands += keys
    specs += [pl.BlockSpec(key.shape, lambda i: (0, 0)) for key in keys]
    if finish:
        outs = jax.ShapeDtypeStruct((rows, heads * VD), jnp.bfloat16)
        out_specs = pl.BlockSpec((rows, step * VD), lambda i: (0, i))
    else:
        outs = [jax.ShapeDtypeStruct((heads * rows, width), jnp.float32) for width in (KV, 256)]
        out_specs = [
            pl.BlockSpec((step * rows, width), lambda i: (i, 0)) for width in (KV, 256)
        ]
    return pl.pallas_call(
        functools.partial(
            attend_kernel, rows, 4 * rows, len(keys), own, bool(earlier), finish
        ),
        grid=(count,),
        in_specs=specs,
        out_specs=out_specs,
        out_shape=outs,
        scratch_shapes=[pltpu.VMEM((key_total, WIDE), jnp.bfloat16)],
        cost_estimate=pl.CostEstimate(
            flops=2 * heads * rows * (key_total * (WIDE + KV) + KV * VD),
            bytes_accessed=2 * heads * (KV * VD + rows * (WIDE + VD)) + 2 * key_total * WIDE,
            transcendentals=heads * rows * key_total,
        ),
        compiler_params=pltpu.CompilerParams(
            vmem_limit_bytes=(16 << 20) + 16 * key_total * WIDE
        ),
        name="attend",
    )(*operands)


def project_kernel(count, offsets, rows_of, finish, added, *refs):
    pieces, chunks = len(offsets), len(rows_of)
    parts = refs[: pieces * chunks]
    weight = refs[pieces * chunks]
    product = None
    for chunk, start in enumerate(rows_of):
        stack = [parts[piece * chunks + chunk][...] for piece in range(pieces)]
        stack = jnp.concatenate(stack, 0) if pieces > 1 else stack[0]
        part = jnp.dot(
            stack,
            weight[start : start + stack.shape[1], :],
            preferred_element_type=jnp.float32,
        )
        product = part if product is None else product + part
    if added:
        product += refs[pieces * chunks + 1][...]
    if not finish:
        refs[-1][...] = product
        return
    out, held, sems = refs[-3:]
    rows = parts[0].shape[0]
    held[...] = product.astype(jnp.bfloat16)
    block = lax.axis_index("seq")
    half = block // 2
    place = jnp.where(block - 2 * half == 0, half, count - 1 - half)
    copies = []
    for i, offset in enumerate(offsets):
        at = lax.rem(place + offset % count, count)
        source = jnp.where(at < count // 2, 2 * at, 2 * (count - 1 - at) + 1)
        copies.append(
            pltpu.make_async_copy(held.at[pl.ds(i * rows, rows), :], out.at[source, 0], sems.at[i])
        )
        copies[-1].start()
    for copy in copies:
        copy.wait()


def project(count, pieces, rows_of, weight, earlier=None, mixed=None, finish=True):
    offsets = [offset for offset, _ in pieces]
    operands = [part for _, parts in pieces for part in parts]
    rows = operands[0].shape[0]
    columns = weight.shape[1]
    total = len(pieces) * rows
    operands.append(weight)
    if earlier is not None:
        operands.append(earlier)
    aliases = {}
    vmem = pl.BlockSpec(memory_space=pltpu.VMEM)
    anywhere = pl.BlockSpec(memory_space=pl.ANY)
    specs = [vmem] * len(operands)
    if finish and mixed is not None:
        aliases = {len(operands): 0}
        operands.append(mixed)
        specs.append(anywhere)
    if finish:
        shape = jax.ShapeDtypeStruct((count, 1, rows, columns), jnp.bfloat16)
        scratch = [
            pltpu.VMEM((total, columns), jnp.bfloat16),
            pltpu.SemaphoreType.DMA((len(pieces),)),
        ]
    else:
        shape = jax.ShapeDtypeStruct((total, columns), jnp.float32)
        scratch = []
    return pl.pallas_call(
        functools.partial(
            project_kernel, count, offsets, rows_of, finish, earlier is not None
        ),
        in_specs=specs,
        out_specs=anywhere if finish else vmem,
        out_shape=shape,
        scratch_shapes=scratch,
        input_output_aliases=aliases,
        compiler_params=pltpu.CompilerParams(vmem_limit_bytes=8 << 20),
        cost_estimate=pl.CostEstimate(
            flops=2 * total * weight.shape[0] * columns,
            bytes_accessed=2 * weight.shape[0] * columns,
            transcendentals=0,
        ),
        name="project",
    )(*operands)


def gather_plan(count):
    moves = []
    bit = count // 2
    slots = [0]
    while bit:
        moves += [(slot, bit) for slot in slots]
        slots += [slot | bit for slot in slots]
        bit //= 2
    return moves


def ring_order(steps):
    names = ["ra1", "la1", "rx1", "lx1", "ry1", "ly1"]
    names += ["ra2", "la2", "rb2", "lb2"]
    return names + [
        way + chunk + str(step) for step in range(3, steps + 1) for chunk in "ab" for way in "rl"
    ]


def layer(queries, latents, latent_gain, key_up, value_up, out_weight):
    seq_count = lax.axis_size("seq")
    head_count = lax.axis_size("head")
    rows = queries.shape[0]
    swap_pairs = [(i, (i + 1) % head_count) for i in range(head_count)]
    everyone = range(seq_count)

    own_keys, half_keys = prepare(latents.T, latent_gain.reshape(1, KV))
    slots = {0: half_keys}
    for slot, bit in gather_plan(seq_count):
        slots[slot | bit] = lax.ppermute(slots[slot], "seq", [(d ^ bit, d) for d in everyone])
    near = [m for m in range(1, seq_count) if m % 2 == 0] + [1]
    far = [m for m in range(2, seq_count) if m % 2 == 1]
    near_keys = jnp.concatenate([slots[m] for m in near], 0)
    middle_keys = jnp.concatenate([slots[m] for m in far[:-1]], 0)
    last_keys = slots[far[-1]]
    near_swap = lax.ppermute(near_keys, "head", swap_pairs)
    middle_swap = lax.ppermute(middle_keys, "head", swap_pairs)
    last_swap = lax.ppermute(last_keys, "head", swap_pairs)

    key_other = lax.ppermute(key_up, "head", swap_pairs)
    value_other = lax.ppermute(value_up, "head", swap_pairs)
    weight_other = lax.ppermute(out_weight, "head", swap_pairs)
    rows_a = lift(queries, key_up, False)
    rows_b = lift(queries, key_other, True)
    count = key_up.shape[0] // 8
    early = [own_keys, near_keys, near_swap, middle_keys]
    late = [middle_swap, last_keys, last_swap]
    keys = early + late
    own = own_keys.shape[0]
    running = attend(rows_a, early, rows, (0, count), own)
    heads_a = attend(rows_a, late, rows, (0, count), 0, value_up, running)
    heads_x = attend(rows_b, keys, rows, (0, count // 2), own, value_other)
    heads_y = attend(rows_b, keys, rows, (count // 2, count - count // 2), own, value_other)

    order = list(range(0, seq_count, 2)) + list(range(seq_count - 1, 0, -2))
    right = [(order[i], order[(i + 1) % seq_count]) for i in everyone]
    left = [(b, a) for a, b in right]
    steps = seq_count // 2
    held = {way + "a0": heads_a for way in "rl"}
    for way in "rl":
        held[way + "x0"], held[way + "y0"] = heads_x, heads_y
    middle = heads_a.shape[1] // 2
    for name in ring_order(steps):
        step = int(name[2:])
        value = held[name[:2] + str(step - 1)]
        if step == steps:
            value = value[:, :middle] if name[0] == "r" else value[:, middle:]
        held[name] = lax.ppermute(value, "seq", right if name[0] == "r" else left)
        if name[1:] == "y1":
            parts = [held[name[0] + "x1"], held[name]]
            held[name[0] + "b1"] = jnp.concatenate(parts, 1)

    def put(mixed, *pieces):
        earlier = project(
            seq_count,
            [(offset, [held[f"{way}a{at}"]]) for offset, way, at in pieces],
            (0,),
            out_weight,
            finish=False,
        )
        return project(
            seq_count,
            [(offset, [held[f"{way}b{at}"]]) for offset, way, at in pieces],
            (0,),
            weight_other,
            earlier,
            mixed,
        )

    earlier = project(seq_count, [(0, [heads_a])], (0,), out_weight, finish=False)
    pieces = [(0, [heads_x, heads_y])]
    mixed = project(seq_count, pieces, (0, middle), weight_other, earlier)
    for step in range(1, steps):
        mixed = put(mixed, (-step, "r", step), (step, "l", step))
    ends = (0, middle)
    pieces = [(steps, [held[f"ra{steps}"], held[f"la{steps}"]])]
    earlier = project(seq_count, pieces, ends, out_weight, finish=False)
    pieces = [(steps, [held[f"rb{steps}"], held[f"lb{steps}"]])]
    return project(seq_count, pieces, ends, weight_other, earlier, mixed)


def solution(mesh):
    placed = (
        P(("groups", "seq", "head"), None),
        P(("groups", "seq"), None),
        P(),
        P("head", None, None),
        P("head", None, None),
        P("head", "seq"),
    )
    return jax.shard_map(
        layer,
        mesh=mesh,
        in_specs=placed,
        out_specs=P("groups", "head", None, "seq"),
        check_vma=False,
    )
```
